512 devices in a mesh: rows: 256 (over z, x, y), modes: 2 (over core).
Axes of the slice: x: 4, y: 8, z: 8, core: 2. Of those that a mesh axis runs over, the one named last changes fastest.
Arguments:
- sample_rows: int32 [256], replicated, may hold values from 0 to 524287, as said below
- basis: float32 [524288, 256], P('rows', 'modes')
- snapshots: float32 [524288, 128], P('rows', 'modes')
Outputs:
- projector: float32 [524288, 256], P('rows', 'modes')
- residual: float32 [524288, 128], P('rows', 'modes')
- residual_rms: float32 [128], P('modes')
The draws below stay inside these ranges and needn't reach their ends.
Inputs may be any that keep to these rules, and one draw needn't show every extreme that they name: `sample_rows`: the indices are distinct. No slab of 2048 consecutive rows (rows j * 2048 to (j + 1) * 2048 - 1) holds more than 8 of them, and some slab holds exactly 8. sampled is row-wise diagonally dominant.
All inputs are finite; a program needn't handle non-finite values.
Results may differ from the reference program's by a relative error of at most 0.000084.
Values sent between devices are 32-bit elements; how exact they have to be, the bound alone decides.
No kernel may reach another device: no remote copies, remote signals or barrier semaphores. Data moves between devices by JAX's collectives and lax.ppermute only.
A program may use at most 128 MiB of HBM per device.

```python
import jax
import jax.numpy as jnp
from jax import lax

K = 256
R_DEV = 2048
S = 128
MOST = 8
NROWS = 524288


def choose_rows(key):
    keyed = jax.random.fold_in(key, 7)
    k_first, k_bias, k_noise, k_offset, k_order = jax.random.split(keyed, 5)
    devices = NROWS // R_DEV
    slot_total = devices * MOST
    slot_ids = jnp.arange(slot_total, dtype=jnp.int32)
    slot_owner = slot_ids // MOST
    first_dev = jax.random.randint(k_first, (), 0, devices, dtype=jnp.int32)
    owner_bias = jax.random.randint(k_bias, (devices,), 0, 4, dtype=jnp.int32)
    noise = jax.random.randint(k_noise, (slot_total,), 0, 131072, dtype=jnp.int32)
    score = (owner_bias[slot_owner] * 32768 + noise) * 4096 + slot_ids
    score = jnp.where(slot_owner == first_dev, 2147483647 - slot_ids, score)
    top_scores, chosen = lax.top_k(score, K)
    owner = chosen // MOST
    within = chosen % MOST
    span = R_DEV // MOST
    offset = within * span + jax.random.randint(k_offset, (K,), 0, span, dtype=jnp.int32)
    picked_rows = owner * R_DEV + offset
    order = jax.random.permutation(k_order, K)
    return picked_rows[order].astype(jnp.int32)


def draw_sample_rows(key, part):
    return choose_rows(key)


def draw_basis(key, part):
    picked_rows = choose_rows(key)
    k_bulk, k_diag, k_sign, k_off, k_ratio = jax.random.split(jax.random.fold_in(key, 11), 5)
    uniform_part = jax.random.uniform(k_off, (K, K), jnp.float32, 0.0, 1.0)
    eye_mask = jnp.eye(K, dtype=jnp.float32)
    bulk = 0.25 * jax.random.normal(k_bulk, (NROWS, K), jnp.float32)
    raw = uniform_part * uniform_part
    load = jax.random.uniform(k_ratio, (K,), jnp.float32, 0.6, 0.9)
    raw = (raw + 1e-06) * (1.0 - eye_mask)
    weights = raw / jnp.sum(raw, axis=1, keepdims=True) * load[:, None]
    magnitude = jax.random.uniform(k_diag, (K,), jnp.float32, 2.0, 4.0)
    sign = jnp.where(jax.random.bernoulli(k_sign, 0.5, (K,)), 1.0, -1.0).astype(jnp.float32)
    block = (magnitude * sign)[:, None] * (weights + eye_mask)
    return bulk.at[picked_rows].set(block)


def draw_snapshots(key, part):
    k_bulk = jax.random.fold_in(jax.random.fold_in(key, 21), 0)
    rising = 1.0 + 2.0 * jnp.arange(NROWS, dtype=jnp.float32) / NROWS
    rough = jax.random.normal(k_bulk, (NROWS, S), jnp.float32)
    return rough * rising[:, None]


def setup_inputs(seed: int = 0) -> dict:
    keys = jax.random.split(jax.random.key(seed), 4)
    sample_rows = draw_sample_rows(jax.random.fold_in(keys[3], 71), 0)
    basis = draw_basis(jax.random.fold_in(keys[3], 71), 0)
    snapshots = draw_snapshots(jax.random.fold_in(keys[3], 71), 0)
    return dict(sample_rows=sample_rows, basis=basis, snapshots=snapshots)


def reference(sample_rows, basis, snapshots):
    sampled = basis[sample_rows]
    picked = snapshots[sample_rows]
    identity = jnp.eye(K, dtype=basis.dtype)
    inverse = jnp.linalg.solve(sampled, identity)
    coeffs = jnp.linalg.solve(sampled, picked)
    projector = jnp.dot(basis, inverse, precision=lax.Precision.HIGHEST)
    residual = snapshots - jnp.dot(basis, coeffs, precision=lax.Precision.HIGHEST)
    residual_rms = jnp.sqrt(lax.optimization_barrier(jnp.sum(residual * residual, axis=0)) / NROWS)
    return (projector, residual, residual_rms)
```

```python
import functools

import jax
import jax.numpy as jnp
from jax import lax
from jax.experimental import pallas as pl
from jax.experimental.pallas import tpu as pltpu
from jax.sharding import Mesh
from jax.sharding import PartitionSpec as P

ROWS = ("rows_0", "rows_1", "rows_2")
F32 = jnp.float32
BF16 = jnp.bfloat16
NT = (((1,), (1,)), ((), ()))
DOUBLINGS = 5
REFINES = 3
TILE = 256
MOST = 8


def dot_once(left, right):
    return jnp.dot(left.astype(BF16), right.astype(BF16), preferred_element_type=F32)

def dot_full(left, right):
    return jnp.dot(left, right, precision=lax.Precision.HIGHEST, preferred_element_type=F32)

def eliminate(matrix, right):
    order, width = matrix.shape
    lanes = lax.broadcasted_iota(jnp.int32, (order, width), 1)
    places = lax.broadcasted_iota(jnp.int32, (order, 1), 0)
    lane = lax.broadcasted_iota(jnp.int32, (1, width), 1)
    def step(k, carry):
        row = matrix[pl.ds(k, 1), :]
        scale = 1.0 / jnp.sum(jnp.where(lane == k, row, 0.0), axis=1, keepdims=True)
        row = row * scale
        answer = right[pl.ds(k, 1), :] * scale
        column = jnp.sum(jnp.where(lanes == k, matrix[...], 0.0), axis=1, keepdims=True)
        column = jnp.where(places == k, 0.0, column)
        matrix[...] = matrix[...] - column * row
        right[...] = right[...] - column * answer
        matrix[pl.ds(k, 1), :] = row
        right[pl.ds(k, 1), :] = answer
        return carry
    lax.fori_loop(0, order, step, 0)

def solve(sampled, right, matrix, answer):
    order = sampled.shape[0]
    i = lax.broadcasted_iota(jnp.int32, (order, order), 0)
    j = lax.broadcasted_iota(jnp.int32, (order, order), 1)
    eye = i == j
    scale = 1.0 / jnp.sum(jnp.where(eye, sampled, 0.0), axis=1, keepdims=True)
    scaled = jnp.where(eye, 1.0, sampled * scale)
    right = right * scale
    power = jnp.where(eye, 0.0, -scaled)
    guess = jnp.where(eye, 1.0, power)
    for _ in range(DOUBLINGS):
        low = power.astype(BF16)
        power = jnp.dot(low, low, preferred_element_type=F32)
        guess = guess + dot_once(power, guess)
    guess = guess.astype(BF16)
    out = jnp.dot(guess, right.astype(BF16), preferred_element_type=F32)
    for _ in range(REFINES):
        fix = jnp.dot(guess, (right - dot_full(scaled, out)).astype(BF16), preferred_element_type=F32)
        out = out + fix
    answer[...] = out
    size = jnp.max(jnp.abs(out), axis=0, keepdims=True)
    change = jnp.max(jnp.abs(fix), axis=0, keepdims=True)
    settled = jnp.min(jnp.where(change <= 1e-4 * size, 1.0, 0.0))
    @pl.when(settled < 0.5)
    def _():
        matrix[...] = scaled
        answer[...] = right
        eliminate(matrix, answer)

def finish_body(table, swapped, own, other, snaps, projector, residual, squares,
                modes_v, snaps_v, projector_v, residual_v, matrix, answer, sem_in, sem_out):
    rows, half = own.shape
    mode = lax.axis_index("modes")
    mine = pl.ds(pl.multiple_of(mode * half, half), half)
    theirs = pl.ds(pl.multiple_of((1 - mode) * half, half), half)
    loads = [
        pltpu.make_async_copy(own, modes_v.at[:, mine], sem_in.at[0]),
        pltpu.make_async_copy(other, modes_v.at[:, theirs], sem_in.at[1]),
        pltpu.make_async_copy(snaps, snaps_v, sem_in.at[2]),
    ]
    for load in loads:
        load.start()
    shape = (table.shape[0], table.shape[2])
    here, there = table[...].reshape(shape), swapped[...].reshape(shape)
    first = jnp.where(mode == 0, here[:, :half], there[:, :half])
    second = jnp.where(mode == 0, there[:, :half], here[:, :half])
    sampled = jnp.concatenate([first, second], axis=1)
    picked = here[:, half:]
    order = sampled.shape[0]
    i = lax.broadcasted_iota(jnp.int32, (order, half), 0)
    j = lax.broadcasted_iota(jnp.int32, (order, half), 1)
    columns = jnp.where(i == j + mode * half, 1.0, 0.0)
    solve(sampled, jnp.concatenate([columns, picked], axis=1), matrix, answer)
    for load in loads:
        load.wait()
    solved = answer[...]
    total = jnp.zeros((snaps.shape[0], TILE), F32)
    stores = []
    for at in range(0, rows, TILE):
        tile = pl.ds(at, TILE)
        product = dot_full(modes_v[tile, :], solved)
        projector_v[tile, :] = product[:, :half]
        left = snaps_v[:, tile] - product[:, half:].T
        residual_v[:, tile] = left
        total = total + left * left
        n = at // TILE
        stores += [
            pltpu.make_async_copy(projector_v.at[tile, :], projector.at[tile, :], sem_out.at[0, n]),
            pltpu.make_async_copy(residual_v.at[:, tile], residual.at[:, tile], sem_out.at[1, n]),
        ]
        stores[-2].start()
        stores[-1].start()
    sums = lax.dot_general(
        jnp.ones((8, TILE), F32), total, NT,
        precision=lax.Precision.HIGHEST, preferred_element_type=F32,
    )
    squares[...] = jnp.broadcast_to(sums[0:1][None], squares.shape)
    for store in stores:
        store.wait()

def finish(table, swapped, own, other, snaps):
    rows, half = own.shape
    shots = snaps.shape[0]
    order = table.shape[0]
    anyspace = pl.BlockSpec(memory_space=pl.ANY)
    vm = pl.BlockSpec(memory_space=pltpu.VMEM)
    return pl.pallas_call(
        finish_body,
        out_shape=(jax.ShapeDtypeStruct((rows, half), F32), jax.ShapeDtypeStruct((shots, rows), F32),
                   jax.ShapeDtypeStruct((order, 1, shots), F32)),
        in_specs=[vm, vm, anyspace, anyspace, anyspace],
        out_specs=(anyspace, anyspace, vm),
        scratch_shapes=[
            pltpu.VMEM((rows, 2 * half), F32), pltpu.VMEM((shots, rows), F32),
            pltpu.VMEM((rows, half), F32), pltpu.VMEM((shots, rows), F32),
            pltpu.VMEM((order, order), F32), pltpu.VMEM((order, half + shots), F32),
            pltpu.SemaphoreType.DMA((3,)), pltpu.SemaphoreType.DMA((2, rows // TILE)),
        ],
        compiler_params=pltpu.CompilerParams(vmem_limit_bytes=32 * 1024 * 1024),
        cost_estimate=pl.CostEstimate(flops=2*rows*256*192, bytes_accessed=6*1024*1024, transcendentals=0),
        name="finish",
    )(table, swapped, own, other, snaps)


def pick_body(sizes, wanted, basis, snaps, table, blocks, strips, staged, place, found, sem):
    rows = basis.shape[0]
    count = table.shape[0]
    half = basis.shape[1]
    slab = 0
    for axis, size in zip(ROWS, sizes):
        slab = slab * size + lax.axis_index(axis)
    start = slab * rows

    def copies(slot, row):
        block = pl.ds(pl.multiple_of(row // 8 * 8, 8), 8)
        strip = pl.ds(pl.multiple_of(row // 128 * 128, 128), 128)
        return (
            pltpu.make_async_copy(basis.at[block, :], blocks.at[slot], sem.at[0, slot]),
            pltpu.make_async_copy(snaps.at[:, strip], strips.at[slot], sem.at[1, slot]),
        )

    for slot in range(MOST):
        found[slot] = 0
        place[slot] = 0

    def look(i, slot):
        row = wanted[i] - start
        held = (row >= 0) & (row < rows) & (slot < MOST)

        @pl.when(held)
        def _():
            found[slot] = row
            place[slot] = i
            for copy in copies(slot, row):
                copy.start()

        return slot + held.astype(jnp.int32)

    used = lax.fori_loop(0, count, look, 0, unroll=8)
    table[...] = jnp.zeros(table.shape, F32)
    for slot in range(MOST):

        @pl.when(slot < used)
        def _():
            for copy in copies(slot, found[slot]):
                copy.wait()

    lanes = lax.broadcasted_iota(jnp.int32, (8, 128), 1)
    for slot in range(MOST):
        row = found[slot]
        hit = jnp.where(lanes == row % 128, 1.0, 0.0)
        shots = lax.dot_general(
            hit, strips[slot], NT, precision=lax.Precision.HIGHEST, preferred_element_type=F32
        )
        staged[slot, :, :half] = blocks[slot, pl.ds(row % 8, 1), :]
        staged[slot, :, half:] = shots[0:1]
    for slot in range(MOST):

        @pl.when(slot < used)
        def _():
            table[pl.ds(place[slot], 1)] = staged[pl.ds(slot, 1)]


def pick(sizes, wanted, basis, snaps):
    half, shots = basis.shape[1], snaps.shape[0]
    anywhere = pl.BlockSpec(memory_space=pl.ANY)
    return pl.pallas_call(
        functools.partial(pick_body, sizes),
        out_shape=jax.ShapeDtypeStruct((wanted.shape[0], 1, half + shots), F32),
        in_specs=[pl.BlockSpec(memory_space=pltpu.SMEM), anywhere, anywhere],
        out_specs=pl.BlockSpec(memory_space=pltpu.VMEM),
        scratch_shapes=[
            pltpu.VMEM((MOST, 8, half), F32),
            pltpu.VMEM((MOST, shots, 128), F32),
            pltpu.VMEM((MOST, 1, half + shots), F32),
            pltpu.SMEM((MOST,), jnp.int32),
            pltpu.SMEM((MOST,), jnp.int32),
            pltpu.SemaphoreType.DMA((2, MOST)),
        ],
        compiler_params=pltpu.CompilerParams(vmem_limit_bytes=60 * 1024 * 1024),
        name="pick",
    )(wanted, basis, snaps)


def share_body(parts, copies):
    copies[...] = jnp.broadcast_to(jnp.sum(parts[...], axis=0, keepdims=True), copies.shape)


def share(parts):
    inside = pl.BlockSpec(memory_space=pltpu.VMEM)
    return pl.pallas_call(
        share_body,
        out_shape=jax.ShapeDtypeStruct(parts.shape, F32),
        in_specs=[inside],
        out_specs=inside,
        compiler_params=pltpu.CompilerParams(vmem_limit_bytes=8 * 1024 * 1024),
        name="share",
    )(parts)


def root_mean_body(total_rows, squares, out):
    out[...] = jnp.sqrt(jnp.sum(squares[...], axis=0) / total_rows)


def root_mean(squares, total_rows):
    inside = pl.BlockSpec(memory_space=pltpu.VMEM)
    return pl.pallas_call(
        functools.partial(root_mean_body, total_rows),
        out_shape=jax.ShapeDtypeStruct((1, squares.shape[2]), F32),
        in_specs=[inside],
        out_specs=inside,
        compiler_params=pltpu.CompilerParams(vmem_limit_bytes=8 * 1024 * 1024),
        name="root_mean",
    )(squares)


def exchange(blocks):
    return lax.all_to_all(blocks, ROWS, 0, 0, tiled=True)


def on_device(sizes, sample_rows, basis, snapshots):
    snaps = snapshots.T
    other = lax.ppermute(basis, "modes", [(0, 1), (1, 0)])
    parts = exchange(pick(sizes, sample_rows, basis, snaps))
    table = exchange(share(parts))
    swapped = lax.ppermute(table, "modes", [(0, 1), (1, 0)])
    projector, residual, squares = finish(table, swapped, basis, other, snaps)
    total_rows = basis.shape[0] * lax.axis_size(ROWS)
    residual_rms = root_mean(exchange(squares), total_rows)
    return (projector, residual.T, residual_rms.reshape(-1))


def solution(mesh):
    sizes = (8, 4, 8)
    torus = Mesh(mesh.devices.reshape(*sizes, mesh.shape["modes"]), (*ROWS, "modes"))
    return jax.shard_map(
        functools.partial(on_device, sizes),
        mesh=torus,
        in_specs=(P(), P(ROWS, "modes"), P(ROWS, "modes")),
        out_specs=(P(ROWS, "modes"), P(ROWS, "modes"), P("modes")),
        check_vma=False,
    )
```

```python
import functools

import jax
import jax.numpy as jnp
from jax import lax
from jax.experimental import pallas as pl
from jax.experimental.pallas import tpu as pltpu
from jax.sharding import Mesh
from jax.sharding import PartitionSpec as P

ROWS = ("rows_0", "rows_1", "rows_2")
F32 = jnp.float32
BF16 = jnp.bfloat16
NT = (((1,), (1,)), ((), ()))
DOUBLINGS = 5
REFINES = 3
TILE = 256
MOST = 8
NARROW = 64
PICK_VMEM = 60 * 1024 * 1024


def dot_once(left, right):
    return jnp.dot(left.astype(BF16), right.astype(BF16), preferred_element_type=F32)

def dot_full(left, right):
    return jnp.dot(left, right, precision=lax.Precision.HIGHEST, preferred_element_type=F32)

def eliminate(matrix, right):
    order, width = matrix.shape
    lanes = lax.broadcasted_iota(jnp.int32, (order, width), 1)
    places = lax.broadcasted_iota(jnp.int32, (order, 1), 0)
    lane = lax.broadcasted_iota(jnp.int32, (1, width), 1)
    def step(k, carry):
        row = matrix[pl.ds(k, 1), :]
        scale = 1.0 / jnp.sum(jnp.where(lane == k, row, 0.0), axis=1, keepdims=True)
        row = row * scale
        answer = right[pl.ds(k, 1), :] * scale
        column = jnp.sum(jnp.where(lanes == k, matrix[...], 0.0), axis=1, keepdims=True)
        column = jnp.where(places == k, 0.0, column)
        matrix[...] = matrix[...] - column * row
        right[...] = right[...] - column * answer
        matrix[pl.ds(k, 1), :] = row
        right[pl.ds(k, 1), :] = answer
        return carry
    lax.fori_loop(0, order, step, 0)

def solve(sampled, right, matrix, answer):
    order = sampled.shape[0]
    i = lax.broadcasted_iota(jnp.int32, (order, order), 0)
    j = lax.broadcasted_iota(jnp.int32, (order, order), 1)
    eye = i == j
    scale = 1.0 / jnp.sum(jnp.where(eye, sampled, 0.0), axis=1, keepdims=True)
    scaled = jnp.where(eye, 1.0, sampled * scale)
    right = right * scale
    power = jnp.where(eye, 0.0, -scaled)
    guess = jnp.where(eye, 1.0, power)
    for _ in range(DOUBLINGS):
        low = power.astype(BF16)
        power = jnp.dot(low, low, preferred_element_type=F32)
        guess = guess + dot_once(power, guess)
    guess = guess.astype(BF16)
    out = jnp.dot(guess, right.astype(BF16), preferred_element_type=F32)
    for _ in range(REFINES):
        fix = jnp.dot(guess, (right - dot_full(scaled, out)).astype(BF16), preferred_element_type=F32)
        out = out + fix
    answer[...] = out
    size = jnp.max(jnp.abs(out), axis=0, keepdims=True)
    change = jnp.max(jnp.abs(fix), axis=0, keepdims=True)
    settled = jnp.min(jnp.where(change <= 1e-4 * size, 1.0, 0.0))
    @pl.when(settled < 0.5)
    def _():
        matrix[...] = scaled
        answer[...] = right
        eliminate(matrix, answer)

def finish_body(modes, swapped, shots, own, other, snaps, projector, residual, squares,
                modes_v, snaps_v, projector_v, residual_v, matrix, answer, sem_in, sem_out):
    rows, half = own.shape
    mode = lax.axis_index("modes")
    mine = pl.ds(pl.multiple_of(mode * half, half), half)
    theirs = pl.ds(pl.multiple_of((1 - mode) * half, half), half)
    loads = [
        pltpu.make_async_copy(own, modes_v.at[:, mine], sem_in.at[0]),
        pltpu.make_async_copy(other, modes_v.at[:, theirs], sem_in.at[1]),
        pltpu.make_async_copy(snaps, snaps_v, sem_in.at[2]),
    ]
    for load in loads:
        load.start()
    here, there = modes[...], swapped[...]
    first = jnp.where(mode == 0, here, there)
    second = jnp.where(mode == 0, there, here)
    sampled = jnp.concatenate([first, second], axis=1)
    picked = shots[...]
    order = sampled.shape[0]
    i = lax.broadcasted_iota(jnp.int32, (order, half), 0)
    j = lax.broadcasted_iota(jnp.int32, (order, half), 1)
    columns = jnp.where(i == j + mode * half, 1.0, 0.0)
    solve(sampled, jnp.concatenate([columns, picked], axis=1), matrix, answer)
    for load in loads:
        load.wait()
    solved = answer[...]
    total = jnp.zeros((snaps.shape[0], TILE), F32)
    stores = []
    for at in range(0, rows, TILE):
        tile = pl.ds(at, TILE)
        product = dot_full(modes_v[tile, :], solved)
        projector_v[tile, :] = product[:, :half]
        left = snaps_v[:, tile] - product[:, half:].T
        residual_v[:, tile] = left
        total = total + left * left
        n = at // TILE
        stores += [
            pltpu.make_async_copy(projector_v.at[tile, :], projector.at[tile, :], sem_out.at[0, n]),
            pltpu.make_async_copy(residual_v.at[:, tile], residual.at[:, tile], sem_out.at[1, n]),
        ]
        stores[-2].start()
        stores[-1].start()
    sums = lax.dot_general(
        jnp.ones((8, TILE), F32), total, NT,
        precision=lax.Precision.HIGHEST, preferred_element_type=F32,
    )
    squares[...] = jnp.broadcast_to(sums[0:1][None], squares.shape)
    for store in stores:
        store.wait()

def finish(modes, swapped, shots, own, other, snaps):
    rows, half = own.shape
    depth = snaps.shape[0]
    order = modes.shape[0]
    anyspace = pl.BlockSpec(memory_space=pl.ANY)
    vm = pl.BlockSpec(memory_space=pltpu.VMEM)
    return pl.pallas_call(
        finish_body,
        out_shape=(jax.ShapeDtypeStruct((rows, half), F32), jax.ShapeDtypeStruct((depth, rows), F32),
                   jax.ShapeDtypeStruct((order, 1, depth), F32)),
        in_specs=[vm, vm, vm, anyspace, anyspace, anyspace],
        out_specs=(anyspace, anyspace, vm),
        scratch_shapes=[
            pltpu.VMEM((rows, 2 * half), F32), pltpu.VMEM((depth, rows), F32),
            pltpu.VMEM((rows, half), F32), pltpu.VMEM((depth, rows), F32),
            pltpu.VMEM((order, order), F32), pltpu.VMEM((order, half + depth), F32),
            pltpu.SemaphoreType.DMA((3,)), pltpu.SemaphoreType.DMA((2, rows // TILE)),
        ],
        compiler_params=pltpu.CompilerParams(vmem_limit_bytes=32 * 1024 * 1024),
        cost_estimate=pl.CostEstimate(flops=2*rows*256*192, bytes_accessed=6*1024*1024, transcendentals=0),
        name="finish",
    )(modes, swapped, shots, own, other, snaps)


def pick_body(sizes, wanted, basis, snaps, sends, places, crowded, blocks, strips, sem):
    rows, half = basis.shape
    shots = snaps.shape[0]
    count = wanted.shape[1]
    deep = sizes[1] * sizes[2]
    start = 0
    for axis, size in zip(ROWS, sizes):
        start = start * size + lax.axis_index(axis)
    start = start * rows

    key = wanted[...]
    local = key % rows
    slab = key // rows
    plane = slab // deep
    line = slab % deep
    across = jnp.broadcast_to(key.astype(F32), (count, count))
    down = across.T
    before = down < across

    def earlier(first):
        same = before & (down >= first.astype(F32))
        return jnp.sum(jnp.where(same, 1.0, 0.0), axis=0, keepdims=True)

    rank = earlier(key - local)
    place = earlier(plane * deep * rows)
    slot = (line * MOST).astype(F32) + rank
    empty = jnp.zeros((8 - 3, count), F32)
    places[...] = jnp.concatenate([place, plane.astype(F32), slot, empty], axis=0)
    crowded[0] = (jnp.max(place) >= NARROW).astype(jnp.int32)

    turn = lax.broadcasted_iota(jnp.int32, (MOST, count), 0).astype(F32)
    held = (key >= start) & (key < start + rows)
    chosen = jnp.where(held & (rank == turn), local.astype(F32) + 1.0, 0.0)
    found = [jnp.sum(chosen[n : n + 1]).astype(jnp.int32) - 1 for n in range(MOST)]

    def copies(n):
        row = jnp.maximum(found[n], 0)
        block = pl.ds(pl.multiple_of(row // 8 * 8, 8), 8)
        strip = pl.ds(pl.multiple_of(row // 128 * 128, 128), 128)
        return (
            pltpu.make_async_copy(basis.at[block, :], blocks.at[n], sem.at[0, n]),
            pltpu.make_async_copy(snaps.at[:, strip], strips.at[n], sem.at[1, n]),
        )

    for n in range(MOST):

        @pl.when(found[n] >= 0)
        def _():
            for copy in copies(n):
                copy.start()

    for n in range(MOST):

        @pl.when(found[n] >= 0)
        def _():
            for copy in copies(n):
                copy.wait()

    lanes = lax.broadcasted_iota(jnp.int32, (shots, 128), 1)
    sublanes = lax.broadcasted_iota(jnp.int32, (MOST, half), 0)
    modes = jnp.zeros((MOST, half), F32)
    columns = jnp.zeros((shots, 128), F32)
    for n in range(MOST):
        row = jnp.maximum(found[n], 0)
        taken = jnp.broadcast_to(blocks[n, pl.ds(row % 8, 1), :], modes.shape)
        modes = jnp.where((sublanes == n) & (found[n] >= 0), taken, modes)
        moved = pltpu.roll(strips[n], (n + 128 - row % 128) % 128, 1)
        columns = jnp.where((lanes == n) & (found[n] >= 0), moved, columns)
    sends[:, :, :half] = jnp.broadcast_to(modes[None], (deep, MOST, half))
    sends[:, :, half:] = jnp.broadcast_to(columns.T[None, :MOST], (deep, MOST, shots))


def pick(sizes, wanted, basis, snaps):
    half, shots = basis.shape[1], snaps.shape[0]
    count = wanted.shape[0]
    outside = pl.BlockSpec(memory_space=pl.ANY)
    inside = pl.BlockSpec(memory_space=pltpu.VMEM)
    return pl.pallas_call(
        functools.partial(pick_body, sizes),
        out_shape=(
            jax.ShapeDtypeStruct((sizes[1] * sizes[2], MOST, half + shots), F32),
            jax.ShapeDtypeStruct((8, count), F32),
            jax.ShapeDtypeStruct((1,), jnp.int32),
        ),
        in_specs=[inside, outside, outside],
        out_specs=(inside, inside, pl.BlockSpec(memory_space=pltpu.SMEM)),
        scratch_shapes=[
            pltpu.VMEM((MOST, 8, half), F32),
            pltpu.VMEM((MOST, shots, 128), F32),
            pltpu.SemaphoreType.DMA((2, MOST)),
        ],
        compiler_params=pltpu.CompilerParams(vmem_limit_bytes=PICK_VMEM),
        name="pick",
    )(wanted.reshape(1, count), basis, snaps)


def dot_exact(choice, right):
    total = None
    for _ in range(3):
        piece = right.astype(BF16)
        right = right - piece.astype(F32)
        part = jnp.dot(choice, piece, preferred_element_type=F32)
        total = part if total is None else total + part
    return total


def pack_body(gathered, places, sends):
    half = sends.shape[2]
    room = sends.shape[1] // 3 * 2
    width = gathered.shape[2]
    count = places.shape[1]
    slots = gathered.shape[0] * gathered.shape[1]
    here = lax.axis_index(ROWS[0]).astype(F32)
    place = jnp.where(places[1:2] == here, places[0:1], -1.0)
    wanted = lax.broadcasted_iota(jnp.int32, (room, count), 0).astype(F32) == place
    slot = lax.broadcasted_iota(jnp.int32, (slots, count), 0).astype(F32) == places[2:3]
    ones = lambda hit: jnp.where(hit, 1.0, 0.0).astype(BF16)
    choice = lax.dot_general(ones(wanted), ones(slot), NT, preferred_element_type=F32)
    packed = dot_exact(choice.astype(BF16), gathered[...].reshape(slots, width))
    pairs = [packed[: room // 2, half:], packed[room // 2 :, half:]]
    packed = jnp.concatenate([packed[:, :half], jnp.concatenate(pairs, axis=1)], axis=0)
    sends[...] = jnp.broadcast_to(packed[None], sends.shape)


def unpack_body(received, places, modes, shots):
    peers = received.shape[0]
    half = modes.shape[1]
    room = received.shape[1] // 3 * 2
    count = places.shape[1]
    address = places[1:2] * room + places[0:1]
    address = jnp.broadcast_to(address, (128, count)).T
    address = jnp.concatenate([address] * (peers * room // 128), axis=1)
    column = lax.broadcasted_iota(jnp.int32, address.shape, 1).astype(F32)
    choice = jnp.where(address == column, 1.0, 0.0).astype(BF16)
    pairs = received[:, room:, :]
    tall = jnp.concatenate([pairs[:, :, : half // 2], pairs[:, :, half // 2 :]], axis=1)
    rows = jnp.concatenate([received[:, :room, :], tall], axis=2)
    table = dot_exact(choice, rows.reshape(peers * room, half + half // 2))
    modes[...] = table[:, :half]
    shots[...] = table[:, half:]


def inside_kernel(body, name, out_shape, *args):
    inside = pl.BlockSpec(memory_space=pltpu.VMEM)
    return pl.pallas_call(
        body,
        out_shape=out_shape,
        in_specs=[inside] * len(args),
        out_specs=jax.tree.map(lambda _: inside, out_shape),
        compiler_params=pltpu.CompilerParams(vmem_limit_bytes=16 * 1024 * 1024),
        name=name,
    )(*args)


def along_planes(planes, half, room, gathered, places):
    width = gathered.shape[2]
    count = places.shape[1]
    shape = jax.ShapeDtypeStruct
    sends = inside_kernel(pack_body, "pack", shape((planes, room + room // 2, half), F32), gathered, places)
    received = lax.all_to_all(sends, ROWS[0], 0, 0, tiled=True)
    out = (shape((count, half), F32), shape((count, width - half), F32))
    return inside_kernel(unpack_body, "unpack", out, received, places)


def root_mean_body(total_rows, squares, out):
    out[...] = jnp.sqrt(jnp.sum(squares[...], axis=0) / total_rows)


def root_mean(squares, total_rows):
    inside = pl.BlockSpec(memory_space=pltpu.VMEM)
    return pl.pallas_call(
        functools.partial(root_mean_body, total_rows),
        out_shape=jax.ShapeDtypeStruct((1, squares.shape[2]), F32),
        in_specs=[inside],
        out_specs=inside,
        compiler_params=pltpu.CompilerParams(vmem_limit_bytes=8 * 1024 * 1024),
        name="root_mean",
    )(squares)


def exchange(blocks):
    return lax.all_to_all(blocks, ROWS, 0, 0, tiled=True)


def on_device(sizes, sample_rows, basis, snapshots):
    snaps = snapshots.T
    half = basis.shape[1]
    other = lax.ppermute(basis, "modes", [(0, 1), (1, 0)])
    sends, places, crowded = pick(sizes, sample_rows, basis, snaps)
    gathered = lax.all_to_all(sends, ROWS[1:], 0, 0, tiled=True)
    narrow, wide = [
        functools.partial(along_planes, sizes[0], half, room)
        for room in (NARROW, sample_rows.shape[0])
    ]
    modes, shots = lax.cond(crowded[0] > 0, wide, narrow, gathered, places)
    swapped = lax.ppermute(modes, "modes", [(0, 1), (1, 0)])
    projector, residual, squares = finish(modes, swapped, shots, basis, other, snaps)
    total_rows = basis.shape[0] * lax.axis_size(ROWS)
    residual_rms = root_mean(exchange(squares), total_rows)
    return (projector, residual.T, residual_rms.reshape(-1))


def solution(mesh):
    sizes = (8, 4, 8)
    torus = Mesh(mesh.devices.reshape(*sizes, mesh.shape["modes"]), (*ROWS, "modes"))
    return jax.shard_map(
        functools.partial(on_device, sizes),
        mesh=torus,
        in_specs=(P(), P(ROWS, "modes"), P(ROWS, "modes")),
        out_specs=(P(ROWS, "modes"), P(ROWS, "modes"), P("modes")),
        check_vma=False,
    )
```

```python
import functools

import jax
import jax.numpy as jnp
from jax import lax
from jax.experimental import pallas as pl
from jax.experimental.pallas import tpu as pltpu
from jax.sharding import Mesh
from jax.sharding import PartitionSpec as P

ROWS = ("rows_0", "rows_1", "rows_2")
F32 = jnp.float32
BF16 = jnp.bfloat16
NT = (((1,), (1,)), ((), ()))
DOUBLINGS = 5
REFINES = 3
TILE = 256
SETTLED = 2e-5
MOST = 8
NARROW = 64
PICK_VMEM = 60 * 1024 * 1024


def dot_once(left, right):
    return jnp.dot(left.astype(BF16), right.astype(BF16), preferred_element_type=F32)


def dot_full(left, right):
    return jnp.dot(left, right, precision=lax.Precision.HIGHEST, preferred_element_type=F32)


def eliminate(matrix, right):
    order, width = matrix.shape
    lanes = lax.broadcasted_iota(jnp.int32, (order, width), 1)
    places = lax.broadcasted_iota(jnp.int32, (order, 1), 0)
    lane = lax.broadcasted_iota(jnp.int32, (1, width), 1)

    def step(k, carry):
        row = matrix[pl.ds(k, 1), :]
        scale = 1.0 / jnp.sum(jnp.where(lane == k, row, 0.0), axis=1, keepdims=True)
        row = row * scale
        answer = right[pl.ds(k, 1), :] * scale
        column = jnp.sum(jnp.where(lanes == k, matrix[...], 0.0), axis=1, keepdims=True)
        column = jnp.where(places == k, 0.0, column)
        matrix[...] = matrix[...] - column * row
        right[...] = right[...] - column * answer
        matrix[pl.ds(k, 1), :] = row
        right[pl.ds(k, 1), :] = answer
        return carry

    lax.fori_loop(0, order, step, 0)


def scaled_rows(modes, swapped):
    mode = lax.axis_index("modes")
    here, there = modes[...], swapped[...]
    first = jnp.where(mode == 0, here, there)
    second = jnp.where(mode == 0, there, here)
    sampled = jnp.concatenate([first, second], axis=1)
    eye = diagonal_of(sampled.shape)
    scale = 1.0 / jnp.sum(jnp.where(eye, sampled, 0.0), axis=1, keepdims=True)
    return jnp.where(eye, 1.0, sampled * scale), scale


def diagonal_of(shape):
    i = lax.broadcasted_iota(jnp.int32, shape, 0)
    j = lax.broadcasted_iota(jnp.int32, shape, 1)
    return i == j


def nearly_inverse(scaled):
    eye = diagonal_of(scaled.shape)
    power = jnp.where(eye, 0.0, -scaled)
    guess = jnp.where(eye, 1.0, power)
    for _ in range(DOUBLINGS):
        low = power.astype(BF16)
        power = jnp.dot(low, low, preferred_element_type=F32)
        guess = guess + dot_once(power, guess)
    return guess.astype(BF16)


def refine(scaled, guess, right, matrix, answer):
    out = jnp.dot(guess, right.astype(BF16), preferred_element_type=F32)
    for _ in range(REFINES):
        left = (right - dot_full(scaled, out)).astype(BF16)
        fix = jnp.dot(guess, left, preferred_element_type=F32)
        out = out + fix
    answer[...] = out
    size = jnp.max(jnp.abs(out), axis=0, keepdims=True)
    change = jnp.max(jnp.abs(fix), axis=0, keepdims=True)
    settled = jnp.min(jnp.where(change <= SETTLED * size, 1.0, 0.0))

    @pl.when(jnp.logical_not(settled > 0.5))
    def _():
        matrix[...] = scaled
        answer[...] = right
        eliminate(matrix, answer)


def load_modes(own, other, modes_v, sem):
    half = own.shape[1]
    mode = lax.axis_index("modes")
    mine = pl.ds(pl.multiple_of(mode * half, half), half)
    theirs = pl.ds(pl.multiple_of((1 - mode) * half, half), half)
    loads = [
        pltpu.make_async_copy(own, modes_v.at[:, mine], sem.at[0]),
        pltpu.make_async_copy(other, modes_v.at[:, theirs], sem.at[1]),
    ]
    for load in loads:
        load.start()
    return loads


def fit_body(
    modes, swapped, shots, own, other, snaps, residual, squares, guess_out,
    modes_v, snaps_v, residual_v, matrix, answer, sem_in, sem_out,
):
    loads = load_modes(own, other, modes_v, sem_in)
    loads.append(pltpu.make_async_copy(snaps, snaps_v, sem_in.at[2]))
    loads[-1].start()
    scaled, scale = scaled_rows(modes, swapped)
    guess = nearly_inverse(scaled)
    guess_out[...] = guess
    refine(scaled, guess, shots[...] * scale, matrix, answer)
    coeffs = answer[...]
    for load in loads:
        load.wait()
    total = jnp.zeros((snaps.shape[0], TILE), F32)
    stores = []
    for n, at in enumerate(range(0, own.shape[0], TILE)):
        tile = pl.ds(at, TILE)
        left = snaps_v[:, tile] - dot_full(modes_v[tile, :], coeffs).T
        residual_v[:, tile] = left
        total = total + left * left
        stores.append(
            pltpu.make_async_copy(residual_v.at[:, tile], residual.at[:, tile], sem_out.at[n])
        )
        stores[-1].start()
    sums = lax.dot_general(
        jnp.ones((8, TILE), F32), total, NT,
        precision=lax.Precision.HIGHEST, preferred_element_type=F32,
    )
    squares[...] = jnp.broadcast_to(sums[0:1][None], squares.shape)
    for store in stores:
        store.wait()


def fit(modes, swapped, shots, own, other, snaps):
    rows, half = own.shape
    depth = snaps.shape[0]
    order = modes.shape[0]
    anywhere = pl.BlockSpec(memory_space=pl.ANY)
    inside = pl.BlockSpec(memory_space=pltpu.VMEM)
    return pl.pallas_call(
        fit_body,
        out_shape=(
            jax.ShapeDtypeStruct((depth, rows), F32),
            jax.ShapeDtypeStruct((order, 1, depth), F32),
            jax.ShapeDtypeStruct((order, order), BF16),
        ),
        in_specs=[inside, inside, inside, anywhere, anywhere, anywhere],
        out_specs=(anywhere, inside, inside),
        scratch_shapes=[
            pltpu.VMEM((rows, 2 * half), F32),
            pltpu.VMEM((depth, rows), F32),
            pltpu.VMEM((depth, rows), F32),
            pltpu.VMEM((order, order), F32),
            pltpu.VMEM((order, depth), F32),
            pltpu.SemaphoreType.DMA((3,)),
            pltpu.SemaphoreType.DMA((rows // TILE,)),
        ],
        compiler_params=pltpu.CompilerParams(vmem_limit_bytes=24 * 1024 * 1024),
        cost_estimate=pl.CostEstimate(
            flops=12 * rows * order * depth, bytes_accessed=16 * rows * half, transcendentals=0
        ),
        name="fit",
    )(modes, swapped, shots, own, other, snaps)


def project_body(
    modes, swapped, guess, own, other, projector,
    modes_v, projector_v, matrix, answer, sem_in, sem_out,
):
    half = own.shape[1]
    loads = load_modes(own, other, modes_v, sem_in)
    scaled, scale = scaled_rows(modes, swapped)
    i = lax.broadcasted_iota(jnp.int32, (scaled.shape[0], half), 0)
    j = lax.broadcasted_iota(jnp.int32, (scaled.shape[0], half), 1)
    columns = jnp.where(i == j + lax.axis_index("modes") * half, scale, 0.0)
    refine(scaled, guess[...], columns, matrix, answer)
    inverse = answer[...]
    for load in loads:
        load.wait()
    stores = []
    for n, at in enumerate(range(0, own.shape[0], TILE)):
        tile = pl.ds(at, TILE)
        projector_v[tile, :] = dot_full(modes_v[tile, :], inverse)
        stores.append(
            pltpu.make_async_copy(projector_v.at[tile, :], projector.at[tile, :], sem_out.at[n])
        )
        stores[-1].start()
    for store in stores:
        store.wait()


def project(modes, swapped, guess, own, other):
    rows, half = own.shape
    order = modes.shape[0]
    anywhere = pl.BlockSpec(memory_space=pl.ANY)
    inside = pl.BlockSpec(memory_space=pltpu.VMEM)
    return pl.pallas_call(
        project_body,
        out_shape=jax.ShapeDtypeStruct((rows, half), F32),
        in_specs=[inside, inside, inside, anywhere, anywhere],
        out_specs=anywhere,
        scratch_shapes=[
            pltpu.VMEM((rows, 2 * half), F32),
            pltpu.VMEM((rows, half), F32),
            pltpu.VMEM((order, order), F32),
            pltpu.VMEM((order, half), F32),
            pltpu.SemaphoreType.DMA((2,)),
            pltpu.SemaphoreType.DMA((rows // TILE,)),
        ],
        compiler_params=pltpu.CompilerParams(vmem_limit_bytes=24 * 1024 * 1024),
        cost_estimate=pl.CostEstimate(
            flops=12 * rows * order * half, bytes_accessed=12 * rows * half, transcendentals=0
        ),
        name="project",
    )(modes, swapped, guess, own, other)


def pick_body(sizes, wanted, basis, snaps, sends, places, crowded, blocks, strips, sem):
    rows, half = basis.shape
    shots = snaps.shape[0]
    count = wanted.shape[1]
    deep = sizes[1] * sizes[2]
    start = 0
    for axis, size in zip(ROWS, sizes):
        start = start * size + lax.axis_index(axis)
    start = start * rows

    key = wanted[...]
    local = key % rows
    slab = key // rows
    plane = slab // deep
    line = slab % deep
    across = jnp.broadcast_to(key.astype(F32), (count, count))
    down = across.T
    before = down < across

    def earlier(first):
        same = before & (down >= first.astype(F32))
        return jnp.sum(jnp.where(same, 1.0, 0.0), axis=0, keepdims=True)

    rank = earlier(key - local)
    place = earlier(plane * deep * rows)
    slot = (line * MOST).astype(F32) + rank
    empty = jnp.zeros((8 - 3, count), F32)
    places[...] = jnp.concatenate([place, plane.astype(F32), slot, empty], axis=0)
    crowded[0] = (jnp.max(place) >= NARROW).astype(jnp.int32)

    turn = lax.broadcasted_iota(jnp.int32, (MOST, count), 0).astype(F32)
    held = (key >= start) & (key < start + rows)
    chosen = jnp.where(held & (rank == turn), local.astype(F32) + 1.0, 0.0)
    found = [jnp.sum(chosen[n : n + 1]).astype(jnp.int32) - 1 for n in range(MOST)]

    def copies(n):
        row = jnp.maximum(found[n], 0)
        block = pl.ds(pl.multiple_of(row // 8 * 8, 8), 8)
        strip = pl.ds(pl.multiple_of(row // 128 * 128, 128), 128)
        return (
            pltpu.make_async_copy(basis.at[block, :], blocks.at[n], sem.at[0, n]),
            pltpu.make_async_copy(snaps.at[:, strip], strips.at[n], sem.at[1, n]),
        )

    for n in range(MOST):

        @pl.when(found[n] >= 0)
        def _():
            for copy in copies(n):
                copy.start()

    for n in range(MOST):

        @pl.when(found[n] >= 0)
        def _():
            for copy in copies(n):
                copy.wait()

    lanes = lax.broadcasted_iota(jnp.int32, (shots, 128), 1)
    sublanes = lax.broadcasted_iota(jnp.int32, (MOST, half), 0)
    modes = jnp.zeros((MOST, half), F32)
    columns = jnp.zeros((shots, 128), F32)
    for n in range(MOST):
        row = jnp.maximum(found[n], 0)
        taken = jnp.broadcast_to(blocks[n, pl.ds(row % 8, 1), :], modes.shape)
        modes = jnp.where((sublanes == n) & (found[n] >= 0), taken, modes)
        moved = pltpu.roll(strips[n], (n + 128 - row % 128) % 128, 1)
        columns = jnp.where((lanes == n) & (found[n] >= 0), moved, columns)
    sends[:, :, :half] = jnp.broadcast_to(modes[None], (deep, MOST, half))
    sends[:, :, half:] = jnp.broadcast_to(columns.T[None, :MOST], (deep, MOST, shots))


def pick(sizes, wanted, basis, snaps):
    half, shots = basis.shape[1], snaps.shape[0]
    count = wanted.shape[0]
    outside = pl.BlockSpec(memory_space=pl.ANY)
    inside = pl.BlockSpec(memory_space=pltpu.VMEM)
    return pl.pallas_call(
        functools.partial(pick_body, sizes),
        out_shape=(
            jax.ShapeDtypeStruct((sizes[1] * sizes[2], MOST, half + shots), F32),
            jax.ShapeDtypeStruct((8, count), F32),
            jax.ShapeDtypeStruct((1,), jnp.int32),
        ),
        in_specs=[inside, outside, outside],
        out_specs=(inside, inside, pl.BlockSpec(memory_space=pltpu.SMEM)),
        scratch_shapes=[
            pltpu.VMEM((MOST, 8, half), F32),
            pltpu.VMEM((MOST, shots, 128), F32),
            pltpu.SemaphoreType.DMA((2, MOST)),
        ],
        compiler_params=pltpu.CompilerParams(vmem_limit_bytes=PICK_VMEM),
        name="pick",
    )(wanted.reshape(1, count), basis, snaps)


def dot_exact(choice, right):
    total = None
    for _ in range(3):
        piece = right.astype(BF16)
        right = right - piece.astype(F32)
        part = jnp.dot(choice, piece, preferred_element_type=F32)
        total = part if total is None else total + part
    return total


def pack_body(gathered, places, sends):
    half = sends.shape[2]
    room = sends.shape[1] // 3 * 2
    width = gathered.shape[2]
    count = places.shape[1]
    slots = gathered.shape[0] * gathered.shape[1]
    here = lax.axis_index(ROWS[0]).astype(F32)
    place = jnp.where(places[1:2] == here, places[0:1], -1.0)
    wanted = lax.broadcasted_iota(jnp.int32, (room, count), 0).astype(F32) == place
    slot = lax.broadcasted_iota(jnp.int32, (slots, count), 0).astype(F32) == places[2:3]
    ones = lambda hit: jnp.where(hit, 1.0, 0.0).astype(BF16)
    choice = lax.dot_general(ones(wanted), ones(slot), NT, preferred_element_type=F32)
    packed = dot_exact(choice.astype(BF16), gathered[...].reshape(slots, width))
    pairs = [packed[: room // 2, half:], packed[room // 2 :, half:]]
    packed = jnp.concatenate([packed[:, :half], jnp.concatenate(pairs, axis=1)], axis=0)
    sends[...] = jnp.broadcast_to(packed[None], sends.shape)


def unpack_body(received, places, modes, shots):
    peers = received.shape[0]
    half = modes.shape[1]
    room = received.shape[1] // 3 * 2
    count = places.shape[1]
    address = places[1:2] * room + places[0:1]
    address = jnp.broadcast_to(address, (128, count)).T
    address = jnp.concatenate([address] * (peers * room // 128), axis=1)
    column = lax.broadcasted_iota(jnp.int32, address.shape, 1).astype(F32)
    choice = jnp.where(address == column, 1.0, 0.0).astype(BF16)
    pairs = received[:, room:, :]
    tall = jnp.concatenate([pairs[:, :, : half // 2], pairs[:, :, half // 2 :]], axis=1)
    rows = jnp.concatenate([received[:, :room, :], tall], axis=2)
    table = dot_exact(choice, rows.reshape(peers * room, half + half // 2))
    modes[...] = table[:, :half]
    shots[...] = table[:, half:]


def inside_kernel(body, out_shape, *args):
    inside = pl.BlockSpec(memory_space=pltpu.VMEM)
    return pl.pallas_call(
        body,
        out_shape=out_shape,
        in_specs=[inside] * len(args),
        out_specs=jax.tree.map(lambda _: inside, out_shape),
        compiler_params=pltpu.CompilerParams(vmem_limit_bytes=16 * 1024 * 1024),
    )(*args)


def along_planes(planes, half, room, gathered, places):
    width = gathered.shape[2]
    count = places.shape[1]
    shape = jax.ShapeDtypeStruct
    sends = inside_kernel(pack_body, shape((planes, room + room // 2, half), F32), gathered, places)
    received = lax.all_to_all(sends, ROWS[0], 0, 0, tiled=True)
    out = (shape((count, half), F32), shape((count, width - half), F32))
    return inside_kernel(unpack_body, out, received, places)


def root_mean_body(total_rows, squares, out):
    out[...] = jnp.sqrt(jnp.sum(squares[...], axis=0) / total_rows)


def root_mean(squares, total_rows):
    inside = pl.BlockSpec(memory_space=pltpu.VMEM)
    return pl.pallas_call(
        functools.partial(root_mean_body, total_rows),
        out_shape=jax.ShapeDtypeStruct((1, squares.shape[2]), F32),
        in_specs=[inside],
        out_specs=inside,
        compiler_params=pltpu.CompilerParams(vmem_limit_bytes=8 * 1024 * 1024),
        name="root_mean",
    )(squares)


def exchange(blocks):
    return lax.all_to_all(blocks, ROWS, 0, 0, tiled=True)


def on_device(sizes, sample_rows, basis, snapshots):
    snaps = snapshots.T
    half = basis.shape[1]
    sends, places, crowded = pick(sizes, sample_rows, basis, snaps)
    gathered = lax.all_to_all(sends, ROWS[1:], 0, 0, tiled=True)
    other = lax.ppermute(basis, "modes", [(0, 1), (1, 0)])
    narrow, wide = [
        functools.partial(along_planes, sizes[0], half, room)
        for room in (NARROW, sample_rows.shape[0])
    ]
    modes, shots = lax.cond(crowded[0] > 0, wide, narrow, gathered, places)
    swapped = lax.ppermute(modes, "modes", [(0, 1), (1, 0)])
    residual, squares, guess = fit(modes, swapped, shots, basis, other, snaps)
    squares = exchange(squares)
    projector = project(modes, swapped, guess, basis, other)
    total_rows = basis.shape[0] * lax.axis_size(ROWS)
    residual_rms = root_mean(squares, total_rows)
    return (projector, residual.T, residual_rms.reshape(-1))


def solution(mesh):
    sizes = (8, 4, 8)
    torus = Mesh(mesh.devices.reshape(*sizes, mesh.shape["modes"]), (*ROWS, "modes"))
    return jax.shard_map(
        functools.partial(on_device, sizes),
        mesh=torus,
        in_specs=(P(), P(ROWS, "modes"), P(ROWS, "modes")),
        out_specs=(P(ROWS, "modes"), P(ROWS, "modes"), P("modes")),
        check_vma=False,
    )
```

```python
import functools

import jax
import jax.numpy as jnp
from jax import lax
from jax.experimental import pallas as pl
from jax.experimental.pallas import tpu as pltpu
from jax.sharding import Mesh
from jax.sharding import PartitionSpec as P

ROWS = ("rows_0", "rows_1", "rows_2")
F32 = jnp.float32
BF16 = jnp.bfloat16
NT = (((1,), (1,)), ((), ()))
DOUBLINGS = 4
REFINES = 2
TILE = 256
SHRINK = 1 / 32
MOST = 8
NARROW = 64
PICK_VMEM = 60 * 1024 * 1024


def dot_once(left, right):
    return jnp.dot(left.astype(BF16), right.astype(BF16), preferred_element_type=F32)


def dot_full(left, right):
    return jnp.dot(left, right, precision=lax.Precision.HIGHEST, preferred_element_type=F32)


def held(array):
    return pltpu.with_memory_space_constraint(array, pltpu.VMEM)


def eliminate(matrix, right):
    order, width = matrix.shape
    lanes = lax.broadcasted_iota(jnp.int32, (order, width), 1)
    places = lax.broadcasted_iota(jnp.int32, (order, 1), 0)
    lane = lax.broadcasted_iota(jnp.int32, (1, width), 1)

    def step(k, carry):
        row = matrix[pl.ds(k, 1), :]
        scale = 1.0 / jnp.sum(jnp.where(lane == k, row, 0.0), axis=1, keepdims=True)
        row = row * scale
        answer = right[pl.ds(k, 1), :] * scale
        column = jnp.sum(jnp.where(lanes == k, matrix[...], 0.0), axis=1, keepdims=True)
        column = jnp.where(places == k, 0.0, column)
        matrix[...] = matrix[...] - column * row
        right[...] = right[...] - column * answer
        matrix[pl.ds(k, 1), :] = row
        right[pl.ds(k, 1), :] = answer
        return carry

    lax.fori_loop(0, order, step, 0)


def scaled_rows(table, swapped, half):
    mode = lax.axis_index("modes")
    here, there = table[:, :half], swapped[:, :half]
    first = jnp.where(mode == 0, here, there)
    second = jnp.where(mode == 0, there, here)
    sampled = jnp.concatenate([first, second], axis=1)
    eye = diagonal_of(sampled.shape)
    scale = 1.0 / jnp.sum(jnp.where(eye, sampled, 0.0), axis=1, keepdims=True)
    return jnp.where(eye, 1.0, sampled * scale), scale


def diagonal_of(shape):
    i = lax.broadcasted_iota(jnp.int32, shape, 0)
    j = lax.broadcasted_iota(jnp.int32, shape, 1)
    return i == j


def nearly_inverse(scaled):
    eye = diagonal_of(scaled.shape)
    power = jnp.where(eye, 0.0, -scaled)
    guess = jnp.where(eye, 1.0, power)
    for _ in range(DOUBLINGS):
        low = power.astype(BF16)
        power = jnp.dot(low, low, preferred_element_type=F32)
        guess = guess + dot_once(power, guess)
    return guess.astype(BF16)


def shrinks(scaled, guess):
    product = None
    rest = scaled
    for _ in range(3):
        piece = rest.astype(BF16)
        rest = rest - piece.astype(F32)
        part = jnp.dot(guess, piece, preferred_element_type=F32)
        product = part if product is None else product + part
    gap = jnp.where(diagonal_of(scaled.shape), 1.0, 0.0) - product
    gap = jnp.sum(jnp.abs(gap), axis=1, keepdims=True)
    rounding = jnp.sum(jnp.abs(guess.astype(F32)), axis=1, keepdims=True) * 2.0**-8
    return jnp.max(gap + rounding) <= SHRINK


def refine(scaled, guess, right):
    out = jnp.dot(guess, right.astype(BF16), preferred_element_type=F32)
    for _ in range(REFINES):
        left = (right - dot_full(scaled, out)).astype(BF16)
        out = out + jnp.dot(guess, left, preferred_element_type=F32)
    return out


def solve(scaled, guess, right, matrix, answer):
    answer[...] = refine(scaled, guess, right)

    @pl.when(jnp.logical_not(shrinks(scaled, guess)))
    def _():
        matrix[...] = scaled
        answer[...] = right
        eliminate(matrix, answer)


def pieces_of(values):
    pieces = []
    for _ in range(3):
        pieces.append(values.astype(BF16))
        values = values - pieces[-1].astype(F32)
    return pieces


def own_first(answer):
    half = answer.shape[0] // 2
    mode = lax.axis_index("modes")
    mine = answer[pl.ds(pl.multiple_of(mode * half, half), half), :]
    theirs = answer[pl.ds(pl.multiple_of((1 - mode) * half, half), half), :]
    return jnp.concatenate([mine, theirs], axis=0)


def fit_body(
    table, swapped, own, other, snaps, residual, squares, system, guess_out,
    matrix, answer, system_v, sem,
):
    scaled, scale = scaled_rows(table, swapped, own.shape[1])
    system_v[...] = jnp.where(diagonal_of(scaled.shape), scale, scaled)
    keep = pltpu.make_async_copy(system_v, system, sem)
    keep.start()
    guess = nearly_inverse(scaled)
    guess_out[...] = guess
    solve(scaled, guess, table[:, own.shape[1] :] * scale, matrix, answer)
    coeffs = own_first(answer)
    depth = coeffs.shape[1]
    spread = jnp.concatenate(pieces_of(coeffs), axis=1)
    total = jnp.zeros((depth, TILE), F32)
    for at in range(0, own.shape[0], TILE):
        tile = pl.ds(at, TILE)
        rows = jnp.concatenate([own[tile, :], other[tile, :]], axis=1)
        product = None
        for piece in pieces_of(rows):
            part = jnp.dot(piece, spread, preferred_element_type=F32)
            product = part if product is None else product + part
        low = product[:, 2 * depth :]
        folded = product[:, : 2 * depth] + jnp.concatenate([low, jnp.zeros_like(low)], axis=1)
        folded = folded.T
        left = snaps[:, tile] - (folded[:depth] + folded[depth:])
        residual[:, tile] = left
        total = total + left * left
    sums = lax.dot_general(
        jnp.ones((8, TILE), F32), total, NT,
        precision=lax.Precision.HIGHEST, preferred_element_type=F32,
    )
    squares[...] = jnp.broadcast_to(sums[0:1][None], squares.shape)
    keep.wait()


def fit(table, swapped, own, other, snaps):
    rows, half = own.shape
    depth = snaps.shape[0]
    order = table.shape[0]
    inside = pl.BlockSpec(memory_space=pltpu.VMEM)
    return pl.pallas_call(
        fit_body,
        out_shape=(
            jax.ShapeDtypeStruct((depth, rows), F32),
            pltpu.HBM((order, 1, depth), F32),
            pltpu.HBM((order, order), F32),
            jax.ShapeDtypeStruct((order, order), BF16),
        ),
        in_specs=[inside] * 5,
        out_specs=(inside, inside, pl.BlockSpec(memory_space=pl.ANY), inside),
        scratch_shapes=[
            pltpu.VMEM((order, order), F32),
            pltpu.VMEM((order, depth), F32),
            pltpu.VMEM((order, order), F32),
            pltpu.SemaphoreType.DMA,
        ],
        compiler_params=pltpu.CompilerParams(vmem_limit_bytes=16 * 1024 * 1024),
        cost_estimate=pl.CostEstimate(
            flops=12 * rows * order * depth, bytes_accessed=16 * rows * half, transcendentals=0
        ),
        name="fit",
    )(held(table), swapped, own, other, snaps)


def project_body(
    system, guess, own, other, residual, projector, residual_out,
    projector_v, matrix, answer, sem_residual, sem_out,
):
    half = own.shape[1]
    keep = pltpu.make_async_copy(residual, residual_out, sem_residual)
    keep.start()
    scaled = system[...]
    eye = diagonal_of(scaled.shape)
    scale = jnp.sum(jnp.where(eye, scaled, 0.0), axis=1, keepdims=True)
    scaled = jnp.where(eye, 1.0, scaled)
    i = lax.broadcasted_iota(jnp.int32, (scaled.shape[0], half), 0)
    j = lax.broadcasted_iota(jnp.int32, (scaled.shape[0], half), 1)
    columns = jnp.where(i == j + lax.axis_index("modes") * half, scale, 0.0)
    solve(scaled, guess[...], columns, matrix, answer)
    inverse = own_first(answer)
    stores = []
    for n, at in enumerate(range(0, own.shape[0], TILE)):
        tile = pl.ds(at, TILE)
        rows = jnp.concatenate([own[tile, :], other[tile, :]], axis=1)
        projector_v[tile, :] = dot_full(rows, inverse)
        stores.append(
            pltpu.make_async_copy(projector_v.at[tile, :], projector.at[tile, :], sem_out.at[n])
        )
        stores[-1].start()
    keep.wait()
    for store in stores:
        store.wait()


def project(system, guess, own, other, residual):
    rows, half = own.shape
    order = system.shape[0]
    anywhere = pl.BlockSpec(memory_space=pl.ANY)
    inside = pl.BlockSpec(memory_space=pltpu.VMEM)
    return pl.pallas_call(
        project_body,
        out_shape=(
            jax.ShapeDtypeStruct((rows, half), F32),
            jax.ShapeDtypeStruct(residual.shape, F32),
        ),
        in_specs=[inside] * 5,
        out_specs=(anywhere, anywhere),
        scratch_shapes=[
            pltpu.VMEM((rows, half), F32),
            pltpu.VMEM((order, order), F32),
            pltpu.VMEM((order, half), F32),
            pltpu.SemaphoreType.DMA,
            pltpu.SemaphoreType.DMA((rows // TILE,)),
        ],
        compiler_params=pltpu.CompilerParams(vmem_limit_bytes=16 * 1024 * 1024),
        cost_estimate=pl.CostEstimate(
            flops=12 * rows * order * half, bytes_accessed=12 * rows * half, transcendentals=0
        ),
        name="project",
    )(system, guess, own, other, residual)


def pick_body(sizes, wanted, basis, snaps, sends, places, crowded, blocks, strips, sem):
    rows, half = basis.shape
    shots = snaps.shape[0]
    count = wanted.shape[1]
    deep = sizes[1] * sizes[2]
    start = 0
    for axis, size in zip(ROWS, sizes):
        start = start * size + lax.axis_index(axis)
    start = start * rows

    key = wanted[...]
    local = key % rows
    slab = key // rows
    plane = slab // deep
    line = slab % deep
    across = jnp.broadcast_to(key.astype(F32), (count, count))
    down = across.T
    before = down < across

    def earlier(first):
        same = before & (down >= first.astype(F32))
        return jnp.sum(jnp.where(same, 1.0, 0.0), axis=0, keepdims=True)

    rank = earlier(key - local)
    place = earlier(plane * deep * rows)
    slot = (line * MOST).astype(F32) + rank
    empty = jnp.zeros((8 - 3, count), F32)
    places[...] = jnp.concatenate([place, plane.astype(F32), slot, empty], axis=0)
    crowded[0] = (jnp.max(place) >= NARROW).astype(jnp.int32)

    turn = lax.broadcasted_iota(jnp.int32, (MOST, count), 0).astype(F32)
    held = (key >= start) & (key < start + rows)
    chosen = jnp.where(held & (rank == turn), local.astype(F32) + 1.0, 0.0)
    found = [jnp.sum(chosen[n : n + 1]).astype(jnp.int32) - 1 for n in range(MOST)]

    def copies(n):
        row = jnp.maximum(found[n], 0)
        block = pl.ds(pl.multiple_of(row // 8 * 8, 8), 8)
        strip = pl.ds(pl.multiple_of(row // 128 * 128, 128), 128)
        return (
            pltpu.make_async_copy(basis.at[block, :], blocks.at[n], sem.at[0, n]),
            pltpu.make_async_copy(snaps.at[:, strip], strips.at[n], sem.at[1, n]),
        )

    for n in range(MOST):

        @pl.when(found[n] >= 0)
        def _():
            for copy in copies(n):
                copy.start()

    for n in range(MOST):

        @pl.when(found[n] >= 0)
        def _():
            for copy in copies(n):
                copy.wait()

    lanes = lax.broadcasted_iota(jnp.int32, (shots, 128), 1)
    sublanes = lax.broadcasted_iota(jnp.int32, (MOST, half), 0)
    modes = jnp.zeros((MOST, half), F32)
    columns = jnp.zeros((shots, 128), F32)
    for n in range(MOST):
        row = jnp.maximum(found[n], 0)
        taken = jnp.broadcast_to(blocks[n, pl.ds(row % 8, 1), :], modes.shape)
        modes = jnp.where((sublanes == n) & (found[n] >= 0), taken, modes)
        moved = pltpu.roll(strips[n], (n + 128 - row % 128) % 128, 1)
        columns = jnp.where((lanes == n) & (found[n] >= 0), moved, columns)
    sends[:, :, :half] = jnp.broadcast_to(modes[None], (deep, MOST, half))
    sends[:, :, half:] = jnp.broadcast_to(columns.T[None, :MOST], (deep, MOST, shots))


def pick(sizes, wanted, basis, snaps):
    half, shots = basis.shape[1], snaps.shape[0]
    count = wanted.shape[0]
    outside = pl.BlockSpec(memory_space=pl.ANY)
    inside = pl.BlockSpec(memory_space=pltpu.VMEM)
    return pl.pallas_call(
        functools.partial(pick_body, sizes),
        out_shape=(
            jax.ShapeDtypeStruct((sizes[1] * sizes[2], MOST, half + shots), F32),
            jax.ShapeDtypeStruct((8, count), F32),
            jax.ShapeDtypeStruct((1,), jnp.int32),
        ),
        in_specs=[inside, outside, outside],
        out_specs=(inside, inside, pl.BlockSpec(memory_space=pltpu.SMEM)),
        scratch_shapes=[
            pltpu.VMEM((MOST, 8, half), F32),
            pltpu.VMEM((MOST, shots, 128), F32),
            pltpu.SemaphoreType.DMA((2, MOST)),
        ],
        compiler_params=pltpu.CompilerParams(vmem_limit_bytes=PICK_VMEM),
        name="pick",
    )(wanted.reshape(1, count), basis, snaps)


def dot_exact(choice, right):
    total = None
    for _ in range(3):
        piece = right.astype(BF16)
        right = right - piece.astype(F32)
        part = jnp.dot(choice, piece, preferred_element_type=F32)
        total = part if total is None else total + part
    return total


def pack_body(gathered, places, sends):
    half = sends.shape[2]
    room = sends.shape[1] // 3 * 2
    width = gathered.shape[2]
    count = places.shape[1]
    slots = gathered.shape[0] * gathered.shape[1]
    here = lax.axis_index(ROWS[0]).astype(F32)
    place = jnp.where(places[1:2] == here, places[0:1], -1.0)
    wanted = lax.broadcasted_iota(jnp.int32, (room, count), 0).astype(F32) == place
    slot = lax.broadcasted_iota(jnp.int32, (slots, count), 0).astype(F32) == places[2:3]
    ones = lambda hit: jnp.where(hit, 1.0, 0.0).astype(BF16)
    choice = lax.dot_general(ones(wanted), ones(slot), NT, preferred_element_type=F32)
    packed = dot_exact(choice.astype(BF16), gathered[...].reshape(slots, width))
    pairs = [packed[: room // 2, half:], packed[room // 2 :, half:]]
    packed = jnp.concatenate([packed[:, :half], jnp.concatenate(pairs, axis=1)], axis=0)
    sends[...] = jnp.broadcast_to(packed[None], sends.shape)


def unpack_body(received, places, table):
    peers, _, half = received.shape
    room = received.shape[1] // 3 * 2
    count = places.shape[1]
    address = places[1:2] * room + places[0:1]
    address = jnp.broadcast_to(address, (128, count)).T
    address = jnp.concatenate([address] * (peers * room // 128), axis=1)
    column = lax.broadcasted_iota(jnp.int32, address.shape, 1).astype(F32)
    choice = jnp.where(address == column, 1.0, 0.0).astype(BF16)
    pairs = received[:, room:, :]
    tall = jnp.concatenate([pairs[:, :, : half // 2], pairs[:, :, half // 2 :]], axis=1)
    rows = jnp.concatenate([received[:, :room, :], tall], axis=2)
    table[...] = dot_exact(choice, rows.reshape(peers * room, half + half // 2))


def inside_kernel(body, out_shape, *args):
    inside = pl.BlockSpec(memory_space=pltpu.VMEM)
    return pl.pallas_call(
        body,
        out_shape=out_shape,
        in_specs=[inside] * len(args),
        out_specs=jax.tree.map(lambda _: inside, out_shape),
        compiler_params=pltpu.CompilerParams(vmem_limit_bytes=16 * 1024 * 1024),
    )(*args)


def along_planes(planes, half, room, gathered, places):
    width = gathered.shape[2]
    count = places.shape[1]
    shape = jax.ShapeDtypeStruct
    sends = inside_kernel(pack_body, shape((planes, room + room // 2, half), F32), gathered, places)
    received = lax.all_to_all(sends, ROWS[0], 0, 0, tiled=True)
    return inside_kernel(unpack_body, shape((count, width), F32), received, places)


def root_mean_body(total_rows, squares, out):
    out[...] = jnp.sqrt(jnp.sum(squares[...], axis=0) / total_rows)


def root_mean(squares, total_rows):
    inside = pl.BlockSpec(memory_space=pltpu.VMEM)
    return pl.pallas_call(
        functools.partial(root_mean_body, total_rows),
        out_shape=jax.ShapeDtypeStruct((1, squares.shape[2]), F32),
        in_specs=[inside],
        out_specs=inside,
        compiler_params=pltpu.CompilerParams(vmem_limit_bytes=8 * 1024 * 1024),
        name="root_mean",
    )(squares)


def exchange(blocks):
    return lax.all_to_all(blocks, ROWS, 0, 0, tiled=True)


def on_device(sizes, sample_rows, basis, snapshots):
    snaps = snapshots.T
    half = basis.shape[1]
    sends, places, crowded = pick(sizes, sample_rows, basis, snaps)
    gathered = lax.all_to_all(sends, ROWS[1:], 0, 0, tiled=True)
    other = lax.ppermute(basis, "modes", [(0, 1), (1, 0)])
    narrow, wide = [
        functools.partial(along_planes, sizes[0], half, room)
        for room in (NARROW, sample_rows.shape[0])
    ]
    table = lax.cond(crowded[0] > 0, wide, narrow, gathered, places)
    swapped = lax.ppermute(table, "modes", [(0, 1), (1, 0)])
    residual, squares, system, guess = fit(table, swapped, basis, other, snaps)
    squares = exchange(squares)
    projector, residual = project(system, guess, basis, other, residual)
    total_rows = basis.shape[0] * lax.axis_size(ROWS)
    residual_rms = root_mean(squares, total_rows)
    return (projector, residual.T, residual_rms.reshape(-1))


def solution(mesh):
    sizes = (8, 4, 8)
    torus = Mesh(mesh.devices.reshape(*sizes, mesh.shape["modes"]), (*ROWS, "modes"))
    return jax.shard_map(
        functools.partial(on_device, sizes),
        mesh=torus,
        in_specs=(P(), P(ROWS, "modes"), P(ROWS, "modes")),
        out_specs=(P(ROWS, "modes"), P(ROWS, "modes"), P("modes")),
        check_vma=False,
    )
```

```python
import functools

import jax
import jax.numpy as jnp
from jax import lax
from jax.experimental import pallas as pl
from jax.experimental.pallas import tpu as pltpu
from jax.sharding import Mesh
from jax.sharding import PartitionSpec as P

ROWS = ("rows_0", "rows_1", "rows_2")
F32 = jnp.float32
BF16 = jnp.bfloat16
NT = (((1,), (1,)), ((), ()))
DOUBLINGS = 4
REFINES = 2
TILE = 256
SHRINK = 1 / 32
MOST = 8
NARROW = 64
PICK_VMEM = 60 * 1024 * 1024


def dot_once(left, right):
    return jnp.dot(left.astype(BF16), right.astype(BF16), preferred_element_type=F32)


def dot_full(left, right):
    return jnp.dot(left, right, precision=lax.Precision.HIGHEST, preferred_element_type=F32)


def held(array):
    return pltpu.with_memory_space_constraint(array, pltpu.VMEM)


def eliminate(matrix, right):
    order, width = matrix.shape
    lanes = lax.broadcasted_iota(jnp.int32, (order, width), 1)
    places = lax.broadcasted_iota(jnp.int32, (order, 1), 0)
    lane = lax.broadcasted_iota(jnp.int32, (1, width), 1)

    def step(k, carry):
        row = matrix[pl.ds(k, 1), :]
        scale = 1.0 / jnp.sum(jnp.where(lane == k, row, 0.0), axis=1, keepdims=True)
        row = row * scale
        answer = right[pl.ds(k, 1), :] * scale
        column = jnp.sum(jnp.where(lanes == k, matrix[...], 0.0), axis=1, keepdims=True)
        column = jnp.where(places == k, 0.0, column)
        matrix[...] = matrix[...] - column * row
        right[...] = right[...] - column * answer
        matrix[pl.ds(k, 1), :] = row
        right[pl.ds(k, 1), :] = answer
        return carry

    lax.fori_loop(0, order, step, 0)


def scaled_rows(sampled):
    eye = diagonal_of(sampled.shape)
    scale = 1.0 / jnp.sum(jnp.where(eye, sampled, 0.0), axis=1, keepdims=True)
    return jnp.where(eye, 1.0, sampled * scale), scale


def diagonal_of(shape):
    i = lax.broadcasted_iota(jnp.int32, shape, 0)
    j = lax.broadcasted_iota(jnp.int32, shape, 1)
    return i == j


def nearly_inverse(scaled):
    eye = diagonal_of(scaled.shape)
    power = jnp.where(eye, 0.0, -scaled)
    guess = jnp.where(eye, 1.0, power)
    for _ in range(DOUBLINGS):
        low = power.astype(BF16)
        power = jnp.dot(low, low, preferred_element_type=F32)
        guess = guess + dot_once(power, guess)
    return guess.astype(BF16)


def shrinks(scaled, guess):
    product = None
    rest = scaled
    for _ in range(3):
        piece = rest.astype(BF16)
        rest = rest - piece.astype(F32)
        part = jnp.dot(guess, piece, preferred_element_type=F32)
        product = part if product is None else product + part
    gap = jnp.where(diagonal_of(scaled.shape), 1.0, 0.0) - product
    gap = jnp.sum(jnp.abs(gap), axis=1, keepdims=True)
    rounding = jnp.sum(jnp.abs(guess.astype(F32)), axis=1, keepdims=True) * 2.0**-8
    return jnp.max(gap + rounding) <= SHRINK


def refine(scaled, guess, right):
    out = jnp.dot(guess, right.astype(BF16), preferred_element_type=F32)
    for _ in range(REFINES):
        left = (right - dot_full(scaled, out)).astype(BF16)
        out = out + jnp.dot(guess, left, preferred_element_type=F32)
    return out


def solve(scaled, guess, right, matrix, answer):
    answer[...] = refine(scaled, guess, right)

    @pl.when(jnp.logical_not(shrinks(scaled, guess)))
    def _():
        matrix[...] = scaled
        answer[...] = right
        eliminate(matrix, answer)


def pieces_of(values):
    pieces = []
    for _ in range(3):
        pieces.append(values.astype(BF16))
        values = values - pieces[-1].astype(F32)
    return pieces


def own_first(answer):
    half = answer.shape[0] // 2
    mode = lax.axis_index("modes")
    mine = answer[pl.ds(pl.multiple_of(mode * half, half), half), :]
    theirs = answer[pl.ds(pl.multiple_of((1 - mode) * half, half), half), :]
    return jnp.concatenate([mine, theirs], axis=0)


def fit_body(
    sampled, shots, own, other, snaps, residual, squares, system, guess_out,
    matrix, answer, system_v, sem,
):
    scaled, scale = scaled_rows(sampled[...])
    system_v[...] = jnp.where(diagonal_of(scaled.shape), scale, scaled)
    keep = pltpu.make_async_copy(system_v, system, sem)
    keep.start()
    guess = nearly_inverse(scaled)
    guess_out[...] = guess
    solve(scaled, guess, shots[...] * scale, matrix, answer)
    coeffs = own_first(answer)
    depth = coeffs.shape[1]
    spread = jnp.concatenate(pieces_of(coeffs), axis=1)
    total = jnp.zeros((depth, TILE), F32)
    for at in range(0, own.shape[0], TILE):
        tile = pl.ds(at, TILE)
        rows = jnp.concatenate([own[tile, :], other[tile, :]], axis=1)
        product = None
        for piece in pieces_of(rows):
            part = jnp.dot(piece, spread, preferred_element_type=F32)
            product = part if product is None else product + part
        low = product[:, 2 * depth :]
        folded = product[:, : 2 * depth] + jnp.concatenate([low, jnp.zeros_like(low)], axis=1)
        folded = folded.T
        left = snaps[:, tile] - (folded[:depth] + folded[depth:])
        residual[:, tile] = left
        total = total + left * left
    sums = lax.dot_general(
        jnp.ones((8, TILE), F32), total, NT,
        precision=lax.Precision.HIGHEST, preferred_element_type=F32,
    )
    squares[...] = jnp.broadcast_to(sums[0:1][None], squares.shape)
    keep.wait()


def fit(sampled, shots, own, other, snaps):
    rows, half = own.shape
    depth = snaps.shape[0]
    order = sampled.shape[0]
    inside = pl.BlockSpec(memory_space=pltpu.VMEM)
    return pl.pallas_call(
        fit_body,
        out_shape=(
            jax.ShapeDtypeStruct((depth, rows), F32),
            pltpu.HBM((order, 1, depth), F32),
            pltpu.HBM((order, order), F32),
            jax.ShapeDtypeStruct((order, order), BF16),
        ),
        in_specs=[inside] * 5,
        out_specs=(inside, inside, pl.BlockSpec(memory_space=pl.ANY), inside),
        scratch_shapes=[
            pltpu.VMEM((order, order), F32),
            pltpu.VMEM((order, depth), F32),
            pltpu.VMEM((order, order), F32),
            pltpu.SemaphoreType.DMA,
        ],
        compiler_params=pltpu.CompilerParams(vmem_limit_bytes=16 * 1024 * 1024),
        cost_estimate=pl.CostEstimate(
            flops=12 * rows * order * depth, bytes_accessed=16 * rows * half, transcendentals=0
        ),
        name="fit",
    )(held(sampled), held(shots), own, other, snaps)


def project_body(
    system, guess, own, other, residual, projector, residual_out,
    projector_v, matrix, answer, sem_residual, sem_out,
):
    half = own.shape[1]
    keep = pltpu.make_async_copy(residual, residual_out, sem_residual)
    keep.start()
    scaled = system[...]
    eye = diagonal_of(scaled.shape)
    scale = jnp.sum(jnp.where(eye, scaled, 0.0), axis=1, keepdims=True)
    scaled = jnp.where(eye, 1.0, scaled)
    i = lax.broadcasted_iota(jnp.int32, (scaled.shape[0], half), 0)
    j = lax.broadcasted_iota(jnp.int32, (scaled.shape[0], half), 1)
    columns = jnp.where(i == j + lax.axis_index("modes") * half, scale, 0.0)
    solve(scaled, guess[...], columns, matrix, answer)
    inverse = own_first(answer)
    stores = []
    for n, at in enumerate(range(0, own.shape[0], TILE)):
        tile = pl.ds(at, TILE)
        rows = jnp.concatenate([own[tile, :], other[tile, :]], axis=1)
        projector_v[tile, :] = dot_full(rows, inverse)
        stores.append(
            pltpu.make_async_copy(projector_v.at[tile, :], projector.at[tile, :], sem_out.at[n])
        )
        stores[-1].start()
    keep.wait()
    for store in stores:
        store.wait()


def project(system, guess, own, other, residual):
    rows, half = own.shape
    order = system.shape[0]
    anywhere = pl.BlockSpec(memory_space=pl.ANY)
    inside = pl.BlockSpec(memory_space=pltpu.VMEM)
    return pl.pallas_call(
        project_body,
        out_shape=(
            jax.ShapeDtypeStruct((rows, half), F32),
            jax.ShapeDtypeStruct(residual.shape, F32),
        ),
        in_specs=[inside] * 5,
        out_specs=(anywhere, anywhere),
        scratch_shapes=[
            pltpu.VMEM((rows, half), F32),
            pltpu.VMEM((order, order), F32),
            pltpu.VMEM((order, half), F32),
            pltpu.SemaphoreType.DMA,
            pltpu.SemaphoreType.DMA((rows // TILE,)),
        ],
        compiler_params=pltpu.CompilerParams(vmem_limit_bytes=16 * 1024 * 1024),
        cost_estimate=pl.CostEstimate(
            flops=12 * rows * order * half, bytes_accessed=12 * rows * half, transcendentals=0
        ),
        name="project",
    )(system, guess, own, other, residual)


def pick_body(sizes, wanted, basis, snaps, sends, places, crowded, blocks, strips, sem):
    rows, half = basis.shape
    shots = snaps.shape[0]
    count = wanted.shape[1]
    deep = sizes[1] * sizes[2]
    start = 0
    for axis, size in zip(ROWS, sizes):
        start = start * size + lax.axis_index(axis)
    start = start * rows

    key = wanted[...]
    local = key % rows
    slab = key // rows
    plane = slab // deep
    line = slab % deep
    across = jnp.broadcast_to(key.astype(F32), (count, count))
    down = across.T
    before = down < across

    def earlier(first):
        same = before & (down >= first.astype(F32))
        return jnp.sum(jnp.where(same, 1.0, 0.0), axis=0, keepdims=True)

    rank = earlier(key - local)
    turn = lax.broadcasted_iota(jnp.int32, (MOST, count), 0).astype(F32)
    held = (key >= start) & (key < start + rows)
    chosen = jnp.where(held & (rank == turn), local.astype(F32) + 1.0, 0.0)
    found = [jnp.sum(chosen[n : n + 1]).astype(jnp.int32) - 1 for n in range(MOST)]

    def copies(n):
        row = jnp.maximum(found[n], 0)
        block = pl.ds(pl.multiple_of(row // 8 * 8, 8), 8)
        strip = pl.ds(pl.multiple_of(row // 128 * 128, 128), 128)
        return (
            pltpu.make_async_copy(basis.at[block, :], blocks.at[n], sem.at[0, n]),
            pltpu.make_async_copy(snaps.at[:, strip], strips.at[n], sem.at[1, n]),
        )

    for n in range(MOST):

        @pl.when(found[n] >= 0)
        def _():
            for copy in copies(n):
                copy.start()

    place = earlier(plane * deep * rows)
    slot = (line * MOST).astype(F32) + rank
    empty = jnp.zeros((8 - 3, count), F32)
    places[...] = jnp.concatenate([place, plane.astype(F32), slot, empty], axis=0)
    crowded[0] = (jnp.max(place) >= NARROW).astype(jnp.int32)

    for n in range(MOST):

        @pl.when(found[n] >= 0)
        def _():
            for copy in copies(n):
                copy.wait()

    lanes = lax.broadcasted_iota(jnp.int32, (shots, 128), 1)
    sublanes = lax.broadcasted_iota(jnp.int32, (MOST, half), 0)
    modes = jnp.zeros((MOST, half), F32)
    columns = jnp.zeros((shots, 128), F32)
    for n in range(MOST):
        row = jnp.maximum(found[n], 0)
        taken = jnp.broadcast_to(blocks[n, pl.ds(row % 8, 1), :], modes.shape)
        modes = jnp.where((sublanes == n) & (found[n] >= 0), taken, modes)
        moved = pltpu.roll(strips[n], (n + 128 - row % 128) % 128, 1)
        columns = jnp.where((lanes == n) & (found[n] >= 0), moved, columns)
    sends[:, :, :half] = jnp.broadcast_to(modes[None], (deep, MOST, half))
    sends[:, :, half:] = jnp.broadcast_to(columns.T[None, :MOST], (deep, MOST, shots))


def pick(sizes, wanted, basis, snaps):
    half, shots = basis.shape[1], snaps.shape[0]
    count = wanted.shape[0]
    outside = pl.BlockSpec(memory_space=pl.ANY)
    inside = pl.BlockSpec(memory_space=pltpu.VMEM)
    return pl.pallas_call(
        functools.partial(pick_body, sizes),
        out_shape=(
            jax.ShapeDtypeStruct((sizes[1] * sizes[2], MOST, half + shots), F32),
            jax.ShapeDtypeStruct((8, count), F32),
            jax.ShapeDtypeStruct((1,), jnp.int32),
        ),
        in_specs=[inside, outside, outside],
        out_specs=(inside, inside, pl.BlockSpec(memory_space=pltpu.SMEM)),
        scratch_shapes=[
            pltpu.VMEM((MOST, 8, half), F32),
            pltpu.VMEM((MOST, shots, 128), F32),
            pltpu.SemaphoreType.DMA((2, MOST)),
        ],
        compiler_params=pltpu.CompilerParams(vmem_limit_bytes=PICK_VMEM),
        name="pick",
    )(wanted.reshape(1, count), basis, snaps)


def dot_exact(choice, right):
    total = None
    for _ in range(3):
        piece = right.astype(BF16)
        right = right - piece.astype(F32)
        part = jnp.dot(choice, piece, preferred_element_type=F32)
        total = part if total is None else total + part
    return total


def pack_body(gathered, places, sends):
    half = sends.shape[2]
    room = sends.shape[1] // 3 * 2
    width = gathered.shape[2]
    count = places.shape[1]
    slots = gathered.shape[0] * gathered.shape[1]
    here = lax.axis_index(ROWS[0]).astype(F32)
    place = jnp.where(places[1:2] == here, places[0:1], -1.0)
    wanted = lax.broadcasted_iota(jnp.int32, (room, count), 0).astype(F32) == place
    slot = lax.broadcasted_iota(jnp.int32, (slots, count), 0).astype(F32) == places[2:3]
    ones = lambda hit: jnp.where(hit, 1.0, 0.0).astype(BF16)
    choice = lax.dot_general(ones(wanted), ones(slot), NT, preferred_element_type=F32)
    packed = dot_exact(choice.astype(BF16), gathered[...].reshape(slots, width))
    pairs = [packed[: room // 2, half:], packed[room // 2 :, half:]]
    packed = jnp.concatenate([packed[:, :half], jnp.concatenate(pairs, axis=1)], axis=0)
    sends[...] = jnp.broadcast_to(packed[None], sends.shape)


def unpack_body(received, places, modes, shots):
    peers, _, half = received.shape
    room = received.shape[1] // 3 * 2
    count = places.shape[1]
    address = places[1:2] * room + places[0:1]
    address = jnp.broadcast_to(address, (128, count)).T
    address = jnp.concatenate([address] * (peers * room // 128), axis=1)
    column = lax.broadcasted_iota(jnp.int32, address.shape, 1).astype(F32)
    choice = jnp.where(address == column, 1.0, 0.0).astype(BF16)
    pairs = received[:, room:, :]
    tall = jnp.concatenate([pairs[:, :, : half // 2], pairs[:, :, half // 2 :]], axis=1)
    rows = jnp.concatenate([received[:, :room, :], tall], axis=2)
    table = dot_exact(choice, rows.reshape(peers * room, half + half // 2))
    modes[...] = table[:, :half]
    shots[...] = table[:, half:]


def inside_kernel(body, out_shape, *args):
    inside = pl.BlockSpec(memory_space=pltpu.VMEM)
    return pl.pallas_call(
        body,
        out_shape=out_shape,
        in_specs=[inside] * len(args),
        out_specs=jax.tree.map(lambda _: inside, out_shape),
        compiler_params=pltpu.CompilerParams(vmem_limit_bytes=16 * 1024 * 1024),
    )(*args)


def along_planes(planes, half, room, gathered, places):
    width = gathered.shape[2]
    count = places.shape[1]
    shape = jax.ShapeDtypeStruct
    sends = inside_kernel(pack_body, shape((planes, room + room // 2, half), F32), gathered, places)
    received = lax.all_to_all(sends, ROWS[0], 0, 0, tiled=True)
    out = (shape((count, half), F32), shape((count, width - half), F32))
    return inside_kernel(unpack_body, out, received, places)


def root_mean_body(total_rows, squares, out):
    out[...] = jnp.sqrt(jnp.sum(squares[...], axis=0) / total_rows)


def root_mean(squares, total_rows):
    inside = pl.BlockSpec(memory_space=pltpu.VMEM)
    return pl.pallas_call(
        functools.partial(root_mean_body, total_rows),
        out_shape=jax.ShapeDtypeStruct((1, squares.shape[2]), F32),
        in_specs=[inside],
        out_specs=inside,
        compiler_params=pltpu.CompilerParams(vmem_limit_bytes=8 * 1024 * 1024),
        name="root_mean",
    )(squares)


def exchange(blocks):
    return lax.all_to_all(blocks, ROWS, 0, 0, tiled=True)


def on_device(sizes, sample_rows, basis, snapshots):
    snaps = snapshots.T
    half = basis.shape[1]
    sends, places, crowded = pick(sizes, sample_rows, basis, snaps)
    gathered = lax.all_to_all(sends, ROWS[1:], 0, 0, tiled=True)
    other = lax.ppermute(basis, "modes", [(0, 1), (1, 0)])
    narrow, wide = [
        functools.partial(along_planes, sizes[0], half, room)
        for room in (NARROW, sample_rows.shape[0])
    ]
    modes, shots = lax.cond(crowded[0] > 0, wide, narrow, gathered, places)
    sampled = lax.all_gather(modes, "modes", axis=1, tiled=True)
    residual, squares, system, guess = fit(sampled, shots, basis, other, snaps)
    squares = exchange(squares)
    projector, residual = project(system, guess, basis, other, residual)
    total_rows = basis.shape[0] * lax.axis_size(ROWS)
    residual_rms = root_mean(squares, total_rows)
    return (projector, residual.T, residual_rms.reshape(-1))


def solution(mesh):
    sizes = (8, 4, 8)
    torus = Mesh(mesh.devices.reshape(*sizes, mesh.shape["modes"]), (*ROWS, "modes"))
    return jax.shard_map(
        functools.partial(on_device, sizes),
        mesh=torus,
        in_specs=(P(), P(ROWS, "modes"), P(ROWS, "modes")),
        out_specs=(P(ROWS, "modes"), P(ROWS, "modes"), P("modes")),
        check_vma=False,
    )
```

```python
import functools

import jax
import jax.numpy as jnp
from jax import lax
from jax.experimental import pallas as pl
from jax.experimental.pallas import tpu as pltpu
from jax.sharding import Mesh
from jax.sharding import PartitionSpec as P

ROWS = ("rows_0", "rows_1", "rows_2")
F32 = jnp.float32
BF16 = jnp.bfloat16
NT = (((1,), (1,)), ((), ()))
DOUBLINGS = 4
REFINES = 2
TILE = 256
SHRINK = 1 / 32
MOST = 8
ROOMS = (48, 64)
PICK_VMEM = 60 * 1024 * 1024


def dot_once(left, right):
    return jnp.dot(left.astype(BF16), right.astype(BF16), preferred_element_type=F32)


def dot_full(left, right):
    return jnp.dot(left, right, precision=lax.Precision.HIGHEST, preferred_element_type=F32)


def held(array):
    return pltpu.with_memory_space_constraint(array, pltpu.VMEM)


def eliminate(matrix, right):
    order, width = matrix.shape
    lanes = lax.broadcasted_iota(jnp.int32, (order, width), 1)
    places = lax.broadcasted_iota(jnp.int32, (order, 1), 0)
    lane = lax.broadcasted_iota(jnp.int32, (1, width), 1)

    def step(k, carry):
        row = matrix[pl.ds(k, 1), :]
        scale = 1.0 / jnp.sum(jnp.where(lane == k, row, 0.0), axis=1, keepdims=True)
        row = row * scale
        answer = right[pl.ds(k, 1), :] * scale
        column = jnp.sum(jnp.where(lanes == k, matrix[...], 0.0), axis=1, keepdims=True)
        column = jnp.where(places == k, 0.0, column)
        matrix[...] = matrix[...] - column * row
        right[...] = right[...] - column * answer
        matrix[pl.ds(k, 1), :] = row
        right[pl.ds(k, 1), :] = answer
        return carry

    lax.fori_loop(0, order, step, 0)


def scaled_rows(sampled):
    eye = diagonal_of(sampled.shape)
    scale = 1.0 / jnp.sum(jnp.where(eye, sampled, 0.0), axis=1, keepdims=True)
    return jnp.where(eye, 1.0, sampled * scale), scale


def diagonal_of(shape):
    i = lax.broadcasted_iota(jnp.int32, shape, 0)
    j = lax.broadcasted_iota(jnp.int32, shape, 1)
    return i == j


def nearly_inverse(scaled):
    eye = diagonal_of(scaled.shape)
    power = jnp.where(eye, 0.0, -scaled)
    guess = jnp.where(eye, 1.0, power)
    for _ in range(DOUBLINGS):
        low = power.astype(BF16)
        power = jnp.dot(low, low, preferred_element_type=F32)
        guess = guess + dot_once(power, guess)
    return guess.astype(BF16)


def shrinks(scaled, guess):
    product = None
    rest = scaled
    for _ in range(3):
        piece = rest.astype(BF16)
        rest = rest - piece.astype(F32)
        part = jnp.dot(guess, piece, preferred_element_type=F32)
        product = part if product is None else product + part
    gap = jnp.where(diagonal_of(scaled.shape), 1.0, 0.0) - product
    gap = jnp.sum(jnp.abs(gap), axis=1, keepdims=True)
    rounding = jnp.sum(jnp.abs(guess.astype(F32)), axis=1, keepdims=True) * 2.0**-8
    return jnp.max(gap + rounding) <= SHRINK


def refine(scaled, guess, right):
    out = jnp.dot(guess, right.astype(BF16), preferred_element_type=F32)
    for _ in range(REFINES):
        left = (right - dot_full(scaled, out)).astype(BF16)
        out = out + jnp.dot(guess, left, preferred_element_type=F32)
    return out


def solve(scaled, guess, right, matrix, answer):
    answer[...] = refine(scaled, guess, right)

    @pl.when(jnp.logical_not(shrinks(scaled, guess)))
    def _():
        matrix[...] = scaled
        answer[...] = right
        eliminate(matrix, answer)


def pieces_of(values):
    pieces = []
    for _ in range(3):
        pieces.append(values.astype(BF16))
        values = values - pieces[-1].astype(F32)
    return pieces


def own_first(answer):
    half = answer.shape[0] // 2
    mode = lax.axis_index("modes")
    mine = answer[pl.ds(pl.multiple_of(mode * half, half), half), :]
    theirs = answer[pl.ds(pl.multiple_of((1 - mode) * half, half), half), :]
    return jnp.concatenate([mine, theirs], axis=0)


def fit_body(
    sampled, shots, own, other, snaps, residual, squares, system, guess_out,
    matrix, answer, system_v, sem,
):
    scaled, scale = scaled_rows(sampled[...])
    system_v[...] = jnp.where(diagonal_of(scaled.shape), scale, scaled)
    keep = pltpu.make_async_copy(system_v, system, sem)
    keep.start()
    guess = nearly_inverse(scaled)
    guess_out[...] = guess
    solve(scaled, guess, shots[...] * scale, matrix, answer)
    coeffs = own_first(answer)
    depth = coeffs.shape[1]
    spread = jnp.concatenate(pieces_of(coeffs), axis=1)
    total = jnp.zeros((depth, TILE), F32)
    for at in range(0, own.shape[0], TILE):
        tile = pl.ds(at, TILE)
        rows = jnp.concatenate([own[tile, :], other[tile, :]], axis=1)
        product = None
        for piece in pieces_of(rows):
            part = jnp.dot(piece, spread, preferred_element_type=F32)
            product = part if product is None else product + part
        low = product[:, 2 * depth :]
        folded = product[:, : 2 * depth] + jnp.concatenate([low, jnp.zeros_like(low)], axis=1)
        folded = folded.T
        left = snaps[:, tile] - (folded[:depth] + folded[depth:])
        residual[:, tile] = left
        total = total + left * left
    sums = lax.dot_general(
        jnp.ones((8, TILE), F32), total, NT,
        precision=lax.Precision.HIGHEST, preferred_element_type=F32,
    )
    squares[...] = jnp.broadcast_to(sums[0:1][None], squares.shape)
    keep.wait()


def fit(sampled, shots, own, other, snaps):
    rows, half = own.shape
    depth = snaps.shape[0]
    order = sampled.shape[0]
    inside = pl.BlockSpec(memory_space=pltpu.VMEM)
    return pl.pallas_call(
        fit_body,
        out_shape=(
            jax.ShapeDtypeStruct((depth, rows), F32),
            pltpu.HBM((order, 1, depth), F32),
            pltpu.HBM((order, order), F32),
            jax.ShapeDtypeStruct((order, order), BF16),
        ),
        in_specs=[inside] * 5,
        out_specs=(inside, inside, pl.BlockSpec(memory_space=pl.ANY), inside),
        scratch_shapes=[
            pltpu.VMEM((order, order), F32),
            pltpu.VMEM((order, depth), F32),
            pltpu.VMEM((order, order), F32),
            pltpu.SemaphoreType.DMA,
        ],
        compiler_params=pltpu.CompilerParams(vmem_limit_bytes=16 * 1024 * 1024),
        cost_estimate=pl.CostEstimate(
            flops=12 * rows * order * depth, bytes_accessed=16 * rows * half, transcendentals=0
        ),
        name="fit",
    )(held(sampled), held(shots), own, other, snaps)


def project_body(
    system, guess, own, other, residual, projector, residual_out,
    projector_v, matrix, answer, sem_residual, sem_out,
):
    half = own.shape[1]
    keep = pltpu.make_async_copy(residual, residual_out, sem_residual)
    keep.start()
    scaled = system[...]
    eye = diagonal_of(scaled.shape)
    scale = jnp.sum(jnp.where(eye, scaled, 0.0), axis=1, keepdims=True)
    scaled = jnp.where(eye, 1.0, scaled)
    i = lax.broadcasted_iota(jnp.int32, (scaled.shape[0], half), 0)
    j = lax.broadcasted_iota(jnp.int32, (scaled.shape[0], half), 1)
    columns = jnp.where(i == j + lax.axis_index("modes") * half, scale, 0.0)
    solve(scaled, guess[...], columns, matrix, answer)
    inverse = own_first(answer)
    stores = []
    for n, at in enumerate(range(0, own.shape[0], TILE)):
        tile = pl.ds(at, TILE)
        rows = jnp.concatenate([own[tile, :], other[tile, :]], axis=1)
        projector_v[tile, :] = dot_full(rows, inverse)
        stores.append(
            pltpu.make_async_copy(projector_v.at[tile, :], projector.at[tile, :], sem_out.at[n])
        )
        stores[-1].start()
    keep.wait()
    for store in stores:
        store.wait()


def project(system, guess, own, other, residual):
    rows, half = own.shape
    order = system.shape[0]
    anywhere = pl.BlockSpec(memory_space=pl.ANY)
    inside = pl.BlockSpec(memory_space=pltpu.VMEM)
    return pl.pallas_call(
        project_body,
        out_shape=(
            jax.ShapeDtypeStruct((rows, half), F32),
            jax.ShapeDtypeStruct(residual.shape, F32),
        ),
        in_specs=[inside] * 5,
        out_specs=(anywhere, anywhere),
        scratch_shapes=[
            pltpu.VMEM((rows, half), F32),
            pltpu.VMEM((order, order), F32),
            pltpu.VMEM((order, half), F32),
            pltpu.SemaphoreType.DMA,
            pltpu.SemaphoreType.DMA((rows // TILE,)),
        ],
        compiler_params=pltpu.CompilerParams(vmem_limit_bytes=16 * 1024 * 1024),
        cost_estimate=pl.CostEstimate(
            flops=12 * rows * order * half, bytes_accessed=12 * rows * half, transcendentals=0
        ),
        name="project",
    )(system, guess, own, other, residual)


def pick_body(sizes, wanted, basis, snaps, sends, places, crowded, blocks, strips, sem):
    rows, half = basis.shape
    shots = snaps.shape[0]
    count = wanted.shape[1]
    deep = sizes[1] * sizes[2]
    start = 0
    for axis, size in zip(ROWS, sizes):
        start = start * size + lax.axis_index(axis)
    start = start * rows

    key = wanted[...]
    local = key % rows
    slab = key // rows
    plane = slab // deep
    line = slab % deep
    across = jnp.broadcast_to(key.astype(F32), (count, count))
    down = across.T
    before = down < across

    def earlier(first):
        same = before & (down >= first.astype(F32))
        return jnp.sum(jnp.where(same, 1.0, 0.0), axis=0, keepdims=True)

    rank = earlier(key - local)
    turn = lax.broadcasted_iota(jnp.int32, (MOST, count), 0).astype(F32)
    held = (key >= start) & (key < start + rows)
    chosen = jnp.where(held & (rank == turn), local.astype(F32) + 1.0, 0.0)
    found = [jnp.sum(chosen[n : n + 1]).astype(jnp.int32) - 1 for n in range(MOST)]

    def copies(n):
        row = jnp.maximum(found[n], 0)
        block = pl.ds(pl.multiple_of(row // 8 * 8, 8), 8)
        strip = pl.ds(pl.multiple_of(row // 128 * 128, 128), 128)
        return (
            pltpu.make_async_copy(basis.at[block, :], blocks.at[n], sem.at[0, n]),
            pltpu.make_async_copy(snaps.at[:, strip], strips.at[n], sem.at[1, n]),
        )

    for n in range(MOST):

        @pl.when(found[n] >= 0)
        def _():
            for copy in copies(n):
                copy.start()

    place = earlier(plane * deep * rows)
    slot = (line * MOST).astype(F32) + rank
    empty = jnp.zeros((8 - 3, count), F32)
    places[...] = jnp.concatenate([place, plane.astype(F32), slot, empty], axis=0)
    most = jnp.max(place)
    crowded[0] = sum((most >= room).astype(jnp.int32) for room in ROOMS)

    for n in range(MOST):

        @pl.when(found[n] >= 0)
        def _():
            for copy in copies(n):
                copy.wait()

    lanes = lax.broadcasted_iota(jnp.int32, (shots, 128), 1)
    sublanes = lax.broadcasted_iota(jnp.int32, (MOST, half), 0)
    modes = jnp.zeros((MOST, half), F32)
    columns = jnp.zeros((shots, 128), F32)
    for n in range(MOST):
        row = jnp.maximum(found[n], 0)
        taken = jnp.broadcast_to(blocks[n, pl.ds(row % 8, 1), :], modes.shape)
        modes = jnp.where((sublanes == n) & (found[n] >= 0), taken, modes)
        moved = pltpu.roll(strips[n], (n + 128 - row % 128) % 128, 1)
        columns = jnp.where((lanes == n) & (found[n] >= 0), moved, columns)
    sends[:, :, :half] = jnp.broadcast_to(modes[None], (deep, MOST, half))
    sends[:, :, half:] = jnp.broadcast_to(columns.T[None, :MOST], (deep, MOST, shots))


def pick(sizes, wanted, basis, snaps):
    half, shots = basis.shape[1], snaps.shape[0]
    count = wanted.shape[0]
    outside = pl.BlockSpec(memory_space=pl.ANY)
    inside = pl.BlockSpec(memory_space=pltpu.VMEM)
    return pl.pallas_call(
        functools.partial(pick_body, sizes),
        out_shape=(
            jax.ShapeDtypeStruct((sizes[1] * sizes[2], MOST, half + shots), F32),
            jax.ShapeDtypeStruct((8, count), F32),
            jax.ShapeDtypeStruct((1,), jnp.int32),
        ),
        in_specs=[inside, outside, outside],
        out_specs=(inside, inside, pl.BlockSpec(memory_space=pltpu.SMEM)),
        scratch_shapes=[
            pltpu.VMEM((MOST, 8, half), F32),
            pltpu.VMEM((MOST, shots, 128), F32),
            pltpu.SemaphoreType.DMA((2, MOST)),
        ],
        compiler_params=pltpu.CompilerParams(vmem_limit_bytes=PICK_VMEM),
        name="pick",
    )(wanted.reshape(1, count), basis, snaps)


def dot_exact(choice, right):
    total = None
    for _ in range(3):
        piece = right.astype(BF16)
        right = right - piece.astype(F32)
        part = jnp.dot(choice, piece, preferred_element_type=F32)
        total = part if total is None else total + part
    return total


def pack_body(gathered, places, sends):
    half = sends.shape[2]
    room = sends.shape[1] // 3 * 2
    width = gathered.shape[2]
    count = places.shape[1]
    slots = gathered.shape[0] * gathered.shape[1]
    here = lax.axis_index(ROWS[0]).astype(F32)
    place = jnp.where(places[1:2] == here, places[0:1], -1.0)
    wanted = lax.broadcasted_iota(jnp.int32, (room, count), 0).astype(F32) == place
    slot = lax.broadcasted_iota(jnp.int32, (slots, count), 0).astype(F32) == places[2:3]
    ones = lambda hit: jnp.where(hit, 1.0, 0.0).astype(BF16)
    choice = lax.dot_general(ones(wanted), ones(slot), NT, preferred_element_type=F32)
    packed = dot_exact(choice.astype(BF16), gathered[...].reshape(slots, width))
    pairs = [packed[: room // 2, half:], packed[room // 2 :, half:]]
    packed = jnp.concatenate([packed[:, :half], jnp.concatenate(pairs, axis=1)], axis=0)
    sends[...] = jnp.broadcast_to(packed[None], sends.shape)


def unpack_body(received, places, modes, shots):
    peers, _, half = received.shape
    room = received.shape[1] // 3 * 2
    count = places.shape[1]
    address = places[1:2] * room + places[0:1]
    address = jnp.broadcast_to(address, (128, count)).T
    address = jnp.concatenate([address] * (peers * room // 128), axis=1)
    column = lax.broadcasted_iota(jnp.int32, address.shape, 1).astype(F32)
    choice = jnp.where(address == column, 1.0, 0.0).astype(BF16)
    pairs = received[:, room:, :]
    tall = jnp.concatenate([pairs[:, :, : half // 2], pairs[:, :, half // 2 :]], axis=1)
    rows = jnp.concatenate([received[:, :room, :], tall], axis=2)
    table = dot_exact(choice, rows.reshape(peers * room, half + half // 2))
    modes[...] = table[:, :half]
    shots[...] = table[:, half:]


def inside_kernel(body, out_shape, *args):
    inside = pl.BlockSpec(memory_space=pltpu.VMEM)
    return pl.pallas_call(
        body,
        out_shape=out_shape,
        in_specs=[inside] * len(args),
        out_specs=jax.tree.map(lambda _: inside, out_shape),
        compiler_params=pltpu.CompilerParams(vmem_limit_bytes=16 * 1024 * 1024),
    )(*args)


def along_planes(planes, half, room, gathered, places):
    width = gathered.shape[2]
    count = places.shape[1]
    shape = jax.ShapeDtypeStruct
    sends = inside_kernel(pack_body, shape((planes, room + room // 2, half), F32), gathered, places)
    received = lax.all_to_all(sends, ROWS[0], 0, 0, tiled=True)
    out = (shape((count, half), F32), shape((count, width - half), F32))
    return inside_kernel(unpack_body, out, received, places)


def root_mean_body(total_rows, squares, out):
    out[...] = jnp.sqrt(jnp.sum(squares[...], axis=0) / total_rows)


def root_mean(squares, total_rows):
    inside = pl.BlockSpec(memory_space=pltpu.VMEM)
    return pl.pallas_call(
        functools.partial(root_mean_body, total_rows),
        out_shape=jax.ShapeDtypeStruct((1, squares.shape[2]), F32),
        in_specs=[inside],
        out_specs=inside,
        compiler_params=pltpu.CompilerParams(vmem_limit_bytes=8 * 1024 * 1024),
        name="root_mean",
    )(squares)


def exchange(blocks):
    return lax.all_to_all(blocks, ROWS, 0, 0, tiled=True)


def on_device(sizes, sample_rows, basis, snapshots):
    snaps = snapshots.T
    half = basis.shape[1]
    sends, places, crowded = pick(sizes, sample_rows, basis, snaps)
    gathered = lax.all_to_all(sends, ROWS[1:], 0, 0, tiled=True)
    other = lax.ppermute(basis, "modes", [(0, 1), (1, 0)])
    branches = [
        functools.partial(along_planes, sizes[0], half, room)
        for room in (*ROOMS, sample_rows.shape[0])
    ]
    modes, shots = lax.switch(crowded[0], branches, gathered, places)
    sampled = lax.all_gather(modes, "modes", axis=1, tiled=True)
    residual, squares, system, guess = fit(sampled, shots, basis, other, snaps)
    squares = exchange(squares)
    projector, residual = project(system, guess, basis, other, residual)
    total_rows = basis.shape[0] * lax.axis_size(ROWS)
    residual_rms = root_mean(squares, total_rows)
    return (projector, residual.T, residual_rms.reshape(-1))


def solution(mesh):
    sizes = (8, 4, 8)
    torus = Mesh(mesh.devices.reshape(*sizes, mesh.shape["modes"]), (*ROWS, "modes"))
    return jax.shard_map(
        functools.partial(on_device, sizes),
        mesh=torus,
        in_specs=(P(), P(ROWS, "modes"), P(ROWS, "modes")),
        out_specs=(P(ROWS, "modes"), P(ROWS, "modes"), P("modes")),
        check_vma=False,
    )
```

```python
import functools

import jax
import jax.numpy as jnp
from jax import lax
from jax.experimental import pallas as pl
from jax.experimental.pallas import tpu as pltpu
from jax.sharding import Mesh
from jax.sharding import PartitionSpec as P

ROWS = ("rows_0", "rows_1", "rows_2")
F32 = jnp.float32
BF16 = jnp.bfloat16
NT = (((1,), (1,)), ((), ()))
DOUBLINGS = 4
REFINES = 2
TILE = 256
SHRINK = 1 / 32
MOST = 8
ROOMS = (48, 64)
PICK_VMEM = 60 * 1024 * 1024


def dot_once(left, right):
    return jnp.dot(left.astype(BF16), right.astype(BF16), preferred_element_type=F32)


def dot_full(left, right):
    return jnp.dot(left, right, precision=lax.Precision.HIGHEST, preferred_element_type=F32)


def held(array):
    return pltpu.with_memory_space_constraint(array, pltpu.VMEM)


def eliminate(matrix, right):
    order, width = matrix.shape
    lanes = lax.broadcasted_iota(jnp.int32, (order, width), 1)
    places = lax.broadcasted_iota(jnp.int32, (order, 1), 0)
    lane = lax.broadcasted_iota(jnp.int32, (1, width), 1)

    def step(k, carry):
        row = matrix[pl.ds(k, 1), :]
        scale = 1.0 / jnp.sum(jnp.where(lane == k, row, 0.0), axis=1, keepdims=True)
        row = row * scale
        answer = right[pl.ds(k, 1), :] * scale
        column = jnp.sum(jnp.where(lanes == k, matrix[...], 0.0), axis=1, keepdims=True)
        column = jnp.where(places == k, 0.0, column)
        matrix[...] = matrix[...] - column * row
        right[...] = right[...] - column * answer
        matrix[pl.ds(k, 1), :] = row
        right[pl.ds(k, 1), :] = answer
        return carry

    lax.fori_loop(0, order, step, 0)


def scaled_rows(sampled):
    eye = diagonal_of(sampled.shape)
    scale = 1.0 / jnp.sum(jnp.where(eye, sampled, 0.0), axis=1, keepdims=True)
    return jnp.where(eye, 1.0, sampled * scale), scale


def diagonal_of(shape):
    i = lax.broadcasted_iota(jnp.int32, shape, 0)
    j = lax.broadcasted_iota(jnp.int32, shape, 1)
    return i == j


def nearly_inverse(scaled):
    eye = diagonal_of(scaled.shape)
    power = jnp.where(eye, 0.0, -scaled)
    guess = jnp.where(eye, 1.0, power)
    for _ in range(DOUBLINGS):
        low = power.astype(BF16)
        power = jnp.dot(low, low, preferred_element_type=F32)
        guess = guess + dot_once(power, guess)
    return guess.astype(BF16)


def pieces_of(values):
    pieces = []
    for _ in range(3):
        pieces.append(values.astype(BF16))
        values = values - pieces[-1].astype(F32)
    return pieces


def dot_pieces(lefts, rights):
    total = None
    for left in lefts:
        part = jnp.dot(left, rights, preferred_element_type=F32)
        total = part if total is None else total + part
    return total


def folded(product):
    width = product.shape[1] // 3
    low = product[:, 2 * width :]
    pair = product[:, : 2 * width] + jnp.concatenate([low, jnp.zeros_like(low)], axis=1)
    return pair[:, :width] + pair[:, width:]


def shrinks(pieces, guess):
    product = None
    for piece in pieces:
        part = jnp.dot(guess, piece, preferred_element_type=F32)
        product = part if product is None else product + part
    gap = jnp.where(diagonal_of(guess.shape), 1.0, 0.0) - product
    gap = jnp.sum(jnp.abs(gap), axis=1, keepdims=True)
    rounding = jnp.sum(jnp.abs(guess.astype(F32)), axis=1, keepdims=True) * 2.0**-8
    return jnp.max(gap + rounding) <= SHRINK


def refine(pieces, guess, right):
    out = jnp.dot(guess, right.astype(BF16), preferred_element_type=F32)
    for _ in range(REFINES):
        spread = jnp.concatenate(pieces_of(out), axis=1)
        left = (right - folded(dot_pieces(pieces, spread))).astype(BF16)
        out = out + jnp.dot(guess, left, preferred_element_type=F32)
    return out


def solve(scaled, guess, right, matrix, answer):
    pieces = pieces_of(scaled)
    sure = shrinks(pieces, guess)
    answer[...] = refine(pieces, guess, right)

    @pl.when(jnp.logical_not(sure))
    def _():
        matrix[...] = scaled
        answer[...] = right
        eliminate(matrix, answer)


def own_first(answer):
    half = answer.shape[0] // 2
    mode = lax.axis_index("modes")
    mine = answer[pl.ds(pl.multiple_of(mode * half, half), half), :]
    theirs = answer[pl.ds(pl.multiple_of((1 - mode) * half, half), half), :]
    return jnp.concatenate([mine, theirs], axis=0)


def fit_body(
    sampled, shots, own, other, snaps, residual, squares, system, guess_out,
    matrix, answer, system_v, sem,
):
    scaled, scale = scaled_rows(sampled[...])
    system_v[...] = jnp.where(diagonal_of(scaled.shape), scale, scaled)
    keep = pltpu.make_async_copy(system_v, system, sem)
    keep.start()
    guess = nearly_inverse(scaled)
    guess_out[...] = guess
    solve(scaled, guess, shots[...] * scale, matrix, answer)
    coeffs = own_first(answer)
    depth = coeffs.shape[1]
    spread = jnp.concatenate(pieces_of(coeffs), axis=1)
    total = jnp.zeros((depth, TILE), F32)
    for at in range(0, own.shape[0], TILE):
        tile = pl.ds(at, TILE)
        rows = jnp.concatenate([own[tile, :], other[tile, :]], axis=1)
        product = None
        for piece in pieces_of(rows):
            part = jnp.dot(piece, spread, preferred_element_type=F32)
            product = part if product is None else product + part
        low = product[:, 2 * depth :]
        folded = product[:, : 2 * depth] + jnp.concatenate([low, jnp.zeros_like(low)], axis=1)
        folded = folded.T
        left = snaps[:, tile] - (folded[:depth] + folded[depth:])
        residual[:, tile] = left
        total = total + left * left
    sums = lax.dot_general(
        jnp.ones((8, TILE), F32), total, NT,
        precision=lax.Precision.HIGHEST, preferred_element_type=F32,
    )
    squares[...] = jnp.broadcast_to(sums[0:1][None], squares.shape)
    keep.wait()


def fit(sampled, shots, own, other, snaps):
    rows, half = own.shape
    depth = snaps.shape[0]
    order = sampled.shape[0]
    inside = pl.BlockSpec(memory_space=pltpu.VMEM)
    return pl.pallas_call(
        fit_body,
        out_shape=(
            jax.ShapeDtypeStruct((depth, rows), F32),
            pltpu.HBM((order, 1, depth), F32),
            pltpu.HBM((order, order), F32),
            jax.ShapeDtypeStruct((order, order), BF16),
        ),
        in_specs=[inside] * 5,
        out_specs=(inside, inside, pl.BlockSpec(memory_space=pl.ANY), inside),
        scratch_shapes=[
            pltpu.VMEM((order, order), F32),
            pltpu.VMEM((order, depth), F32),
            pltpu.VMEM((order, order), F32),
            pltpu.SemaphoreType.DMA,
        ],
        compiler_params=pltpu.CompilerParams(vmem_limit_bytes=16 * 1024 * 1024),
        cost_estimate=pl.CostEstimate(
            flops=12 * rows * order * depth, bytes_accessed=16 * rows * half, transcendentals=0
        ),
        name="fit",
    )(held(sampled), held(shots), own, other, snaps)


def project_body(
    system, guess, own, other, residual, projector, residual_out,
    projector_v, matrix, answer, sem_residual, sem_out,
):
    half = own.shape[1]
    keep = pltpu.make_async_copy(residual, residual_out, sem_residual)
    keep.start()
    scaled = system[...]
    eye = diagonal_of(scaled.shape)
    scale = jnp.sum(jnp.where(eye, scaled, 0.0), axis=1, keepdims=True)
    scaled = jnp.where(eye, 1.0, scaled)
    i = lax.broadcasted_iota(jnp.int32, (scaled.shape[0], half), 0)
    j = lax.broadcasted_iota(jnp.int32, (scaled.shape[0], half), 1)
    columns = jnp.where(i == j + lax.axis_index("modes") * half, scale, 0.0)
    solve(scaled, guess[...], columns, matrix, answer)
    inverse = own_first(answer)
    stores = []
    for n, at in enumerate(range(0, own.shape[0], TILE)):
        tile = pl.ds(at, TILE)
        rows = jnp.concatenate([own[tile, :], other[tile, :]], axis=1)
        projector_v[tile, :] = dot_full(rows, inverse)
        stores.append(
            pltpu.make_async_copy(projector_v.at[tile, :], projector.at[tile, :], sem_out.at[n])
        )
        stores[-1].start()
    keep.wait()
    for store in stores:
        store.wait()


def project(system, guess, own, other, residual):
    rows, half = own.shape
    order = system.shape[0]
    anywhere = pl.BlockSpec(memory_space=pl.ANY)
    inside = pl.BlockSpec(memory_space=pltpu.VMEM)
    return pl.pallas_call(
        project_body,
        out_shape=(
            jax.ShapeDtypeStruct((rows, half), F32),
            jax.ShapeDtypeStruct(residual.shape, F32),
        ),
        in_specs=[inside] * 5,
        out_specs=(anywhere, anywhere),
        scratch_shapes=[
            pltpu.VMEM((rows, half), F32),
            pltpu.VMEM((order, order), F32),
            pltpu.VMEM((order, half), F32),
            pltpu.SemaphoreType.DMA,
            pltpu.SemaphoreType.DMA((rows // TILE,)),
        ],
        compiler_params=pltpu.CompilerParams(vmem_limit_bytes=16 * 1024 * 1024),
        cost_estimate=pl.CostEstimate(
            flops=12 * rows * order * half, bytes_accessed=12 * rows * half, transcendentals=0
        ),
        name="project",
    )(system, guess, own, other, residual)


def counter(key):
    count = key.shape[1]
    across = jnp.broadcast_to(key.astype(F32), (count, count))
    down = across.T
    before = down < across

    def earlier(first):
        same = before & (down >= first.astype(F32))
        return jnp.sum(jnp.where(same, 1.0, 0.0), axis=0, keepdims=True)

    return earlier


def plan_body(rows, deep, wanted, places, crowded):
    key = wanted[...]
    slab = key // rows
    plane = slab // deep
    line = slab % deep
    earlier = counter(key)
    place = earlier(plane * deep * rows)
    slot = (line * MOST).astype(F32) + earlier(slab * rows)
    empty = jnp.zeros((8 - 3, key.shape[1]), F32)
    places[...] = jnp.concatenate([place, plane.astype(F32), slot, empty], axis=0)
    most = jnp.max(place)
    crowded[0] = sum((most >= room).astype(jnp.int32) for room in ROOMS)


def plan(sizes, rows, wanted):
    count = wanted.shape[0]
    inside = pl.BlockSpec(memory_space=pltpu.VMEM)
    return pl.pallas_call(
        functools.partial(plan_body, rows, sizes[1] * sizes[2]),
        out_shape=(
            jax.ShapeDtypeStruct((8, count), F32),
            jax.ShapeDtypeStruct((1,), jnp.int32),
        ),
        in_specs=[inside],
        out_specs=(inside, pl.BlockSpec(memory_space=pltpu.SMEM)),
        compiler_params=pltpu.CompilerParams(vmem_limit_bytes=8 * 1024 * 1024),
        name="plan",
    )(wanted.reshape(1, count))


def pick_body(sizes, wanted, basis, snaps, sends, blocks, strips, sem):
    rows, half = basis.shape
    shots = snaps.shape[0]
    count = wanted.shape[1]
    deep = sizes[1] * sizes[2]
    start = 0
    for axis, size in zip(ROWS, sizes):
        start = start * size + lax.axis_index(axis)
    start = start * rows

    key = wanted[...]
    local = key % rows
    rank = counter(key)(key - local)
    turn = lax.broadcasted_iota(jnp.int32, (MOST, count), 0).astype(F32)
    held = (key >= start) & (key < start + rows)
    chosen = jnp.where(held & (rank == turn), local.astype(F32) + 1.0, 0.0)
    found = [jnp.sum(chosen[n : n + 1]).astype(jnp.int32) - 1 for n in range(MOST)]

    def copies(n):
        row = jnp.maximum(found[n], 0)
        block = pl.ds(pl.multiple_of(row // 8 * 8, 8), 8)
        strip = pl.ds(pl.multiple_of(row // 128 * 128, 128), 128)
        return (
            pltpu.make_async_copy(basis.at[block, :], blocks.at[n], sem.at[0, n]),
            pltpu.make_async_copy(snaps.at[:, strip], strips.at[n], sem.at[1, n]),
        )

    for n in range(MOST):

        @pl.when(found[n] >= 0)
        def _():
            for copy in copies(n):
                copy.start()

    for n in range(MOST):

        @pl.when(found[n] >= 0)
        def _():
            for copy in copies(n):
                copy.wait()

    lanes = lax.broadcasted_iota(jnp.int32, (shots, 128), 1)
    sublanes = lax.broadcasted_iota(jnp.int32, (MOST, half), 0)
    modes = jnp.zeros((MOST, half), F32)
    columns = jnp.zeros((shots, 128), F32)
    for n in range(MOST):
        row = jnp.maximum(found[n], 0)
        taken = jnp.broadcast_to(blocks[n, pl.ds(row % 8, 1), :], modes.shape)
        modes = jnp.where((sublanes == n) & (found[n] >= 0), taken, modes)
        moved = pltpu.roll(strips[n], (n + 128 - row % 128) % 128, 1)
        columns = jnp.where((lanes == n) & (found[n] >= 0), moved, columns)
    sends[:, :, :half] = jnp.broadcast_to(modes[None], (deep, MOST, half))
    sends[:, :, half:] = jnp.broadcast_to(columns.T[None, :MOST], (deep, MOST, shots))


def pick(sizes, wanted, basis, snaps):
    half, shots = basis.shape[1], snaps.shape[0]
    count = wanted.shape[0]
    outside = pl.BlockSpec(memory_space=pl.ANY)
    inside = pl.BlockSpec(memory_space=pltpu.VMEM)
    return pl.pallas_call(
        functools.partial(pick_body, sizes),
        out_shape=jax.ShapeDtypeStruct((sizes[1] * sizes[2], MOST, half + shots), F32),
        in_specs=[inside, outside, outside],
        out_specs=inside,
        scratch_shapes=[
            pltpu.VMEM((MOST, 8, half), F32),
            pltpu.VMEM((MOST, shots, 128), F32),
            pltpu.SemaphoreType.DMA((2, MOST)),
        ],
        compiler_params=pltpu.CompilerParams(vmem_limit_bytes=PICK_VMEM),
        name="pick",
    )(wanted.reshape(1, count), basis, snaps)


def dot_exact(choice, right):
    total = None
    for _ in range(3):
        piece = right.astype(BF16)
        right = right - piece.astype(F32)
        part = jnp.dot(choice, piece, preferred_element_type=F32)
        total = part if total is None else total + part
    return total


def pack_body(gathered, places, sends):
    half = sends.shape[2]
    room = sends.shape[1] // 3 * 2
    width = gathered.shape[2]
    count = places.shape[1]
    slots = gathered.shape[0] * gathered.shape[1]
    here = lax.axis_index(ROWS[0]).astype(F32)
    place = jnp.where(places[1:2] == here, places[0:1], -1.0)
    wanted = lax.broadcasted_iota(jnp.int32, (room, count), 0).astype(F32) == place
    slot = lax.broadcasted_iota(jnp.int32, (slots, count), 0).astype(F32) == places[2:3]
    ones = lambda hit: jnp.where(hit, 1.0, 0.0).astype(BF16)
    choice = lax.dot_general(ones(wanted), ones(slot), NT, preferred_element_type=F32)
    packed = dot_exact(choice.astype(BF16), gathered[...].reshape(slots, width))
    pairs = [packed[: room // 2, half:], packed[room // 2 :, half:]]
    packed = jnp.concatenate([packed[:, :half], jnp.concatenate(pairs, axis=1)], axis=0)
    sends[...] = jnp.broadcast_to(packed[None], sends.shape)


def unpack_body(received, places, modes, shots):
    peers, _, half = received.shape
    room = received.shape[1] // 3 * 2
    count = places.shape[1]
    address = places[1:2] * room + places[0:1]
    address = jnp.broadcast_to(address, (128, count)).T
    address = jnp.concatenate([address] * (peers * room // 128), axis=1)
    column = lax.broadcasted_iota(jnp.int32, address.shape, 1).astype(F32)
    choice = jnp.where(address == column, 1.0, 0.0).astype(BF16)
    pairs = received[:, room:, :]
    tall = jnp.concatenate([pairs[:, :, : half // 2], pairs[:, :, half // 2 :]], axis=1)
    rows = jnp.concatenate([received[:, :room, :], tall], axis=2)
    table = dot_exact(choice, rows.reshape(peers * room, half + half // 2))
    modes[...] = table[:, :half]
    shots[...] = table[:, half:]


def inside_kernel(body, out_shape, *args):
    inside = pl.BlockSpec(memory_space=pltpu.VMEM)
    return pl.pallas_call(
        body,
        out_shape=out_shape,
        in_specs=[inside] * len(args),
        out_specs=jax.tree.map(lambda _: inside, out_shape),
        compiler_params=pltpu.CompilerParams(vmem_limit_bytes=16 * 1024 * 1024),
    )(*args)


def along_planes(planes, half, room, gathered, places):
    width = gathered.shape[2]
    count = places.shape[1]
    shape = jax.ShapeDtypeStruct
    sends = inside_kernel(pack_body, shape((planes, room + room // 2, half), F32), gathered, places)
    received = lax.all_to_all(sends, ROWS[0], 0, 0, tiled=True)
    out = (shape((count, half), F32), shape((count, width - half), F32))
    return inside_kernel(unpack_body, out, received, places)


def root_mean_body(total_rows, squares, out):
    out[...] = jnp.sqrt(jnp.sum(squares[...], axis=0) / total_rows)


def root_mean(squares, total_rows):
    inside = pl.BlockSpec(memory_space=pltpu.VMEM)
    return pl.pallas_call(
        functools.partial(root_mean_body, total_rows),
        out_shape=jax.ShapeDtypeStruct((1, squares.shape[2]), F32),
        in_specs=[inside],
        out_specs=inside,
        compiler_params=pltpu.CompilerParams(vmem_limit_bytes=8 * 1024 * 1024),
        name="root_mean",
    )(squares)


def exchange(blocks):
    return lax.all_to_all(blocks, ROWS, 0, 0, tiled=True)


def on_device(sizes, sample_rows, basis, snapshots):
    snaps = snapshots.T
    half = basis.shape[1]
    sends = pick(sizes, sample_rows, basis, snaps)
    gathered = lax.all_to_all(sends, ROWS[1:], 0, 0, tiled=True)
    places, crowded = plan(sizes, basis.shape[0], sample_rows)
    other = lax.ppermute(basis, "modes", [(0, 1), (1, 0)])
    branches = [
        functools.partial(along_planes, sizes[0], half, room)
        for room in (*ROOMS, sample_rows.shape[0])
    ]
    modes, shots = lax.switch(crowded[0], branches, gathered, places)
    sampled = lax.all_gather(modes, "modes", axis=1, tiled=True)
    residual, squares, system, guess = fit(sampled, shots, basis, other, snaps)
    squares = exchange(squares)
    projector, residual = project(system, guess, basis, other, residual)
    total_rows = basis.shape[0] * lax.axis_size(ROWS)
    residual_rms = root_mean(squares, total_rows)
    return (projector, residual.T, residual_rms.reshape(-1))


def solution(mesh):
    sizes = (8, 4, 8)
    torus = Mesh(mesh.devices.reshape(*sizes, mesh.shape["modes"]), (*ROWS, "modes"))
    return jax.shard_map(
        functools.partial(on_device, sizes),
        mesh=torus,
        in_specs=(P(), P(ROWS, "modes"), P(ROWS, "modes")),
        out_specs=(P(ROWS, "modes"), P(ROWS, "modes"), P("modes")),
        check_vma=False,
    )
```
